32 devices in a mesh: dp: 1 (over z), cp: 32 (over y, x, core).
Axes of the slice: x: 4, y: 4, z: 1, core: 2. Of those that a mesh axis runs over, the one named last changes fastest.
The devices are a block of a 4x4x8 slice.
Arguments:
- x_in: bfloat16 [1, 8192, 8192], P('dp', 'cp')
- seg_ids: int32 [8192], P(('dp', 'cp'))
- positions: int32 [8192], P(('dp', 'cp'))
- attn_gain: bfloat16 [8192], replicated
- w_q: bfloat16 [8192, 1024], replicated
- w_k: bfloat16 [8192, 128], replicated
- w_v: bfloat16 [8192, 128], replicated
- w_o: bfloat16 [1024, 8192], replicated
- mlp_gain: bfloat16 [8192], replicated
- w_gate: bfloat16 [8192, 3584], replicated
- w_up: bfloat16 [8192, 3584], replicated
- w_down: bfloat16 [3584, 8192], replicated
Outputs:
- output 1: bfloat16 [1, 8192, 8192], P('dp', 'cp')
- output 2: bfloat16 [8192, 1, 128], P(('dp', 'cp'))
- output 3: bfloat16 [8192, 1, 128], P(('dp', 'cp'))
All inputs are finite; a program needn't handle non-finite values.
Results may differ from the reference program's by a relative error of at most 0.0112256.
Values are sent between devices in bfloat16 or wider.
A program may use at most 768 MiB of HBM per device.

```python
import jax
import jax.numpy as jnp
from jax import lax

MODEL_DIM = 8192
HEADS = 8
KV_HEADS = 1
HEAD_DIM = 128
FF_DIM = 3584
TOKENS_DEV = 256
CP_SIZE = 32
NUM_PROMPTS = 8
ATT_ROWS = 8

SEQ_LEN = TOKENS_DEV * CP_SIZE
CHUNK_ROWS = TOKENS_DEV // 2
GROUP_REP = HEADS // KV_HEADS
ROPE_THETA = 500000.0
ROPE_FACTOR = 8.0
LOW_FREQ = 1.0
HIGH_FREQ = 4.0
ORIG_CTX = 8192.0
NORM_EPS = 1e-5
NEG_BIG = -1e30


def rope_freqs():
    exponent = jnp.arange(0, HEAD_DIM, 2).astype(jnp.float32) / HEAD_DIM
    inv_freq = 1.0 / (ROPE_THETA ** exponent)
    wavelen = 2.0 * jnp.pi / inv_freq
    smooth = jnp.clip((ORIG_CTX / wavelen - LOW_FREQ) / (HIGH_FREQ - LOW_FREQ), 0.0, 1.0)
    return (1.0 - smooth) * inv_freq / ROPE_FACTOR + smooth * inv_freq


def apply_rope(tensor, cos_t, sin_t):
    half = tensor.shape[-1] // 2
    first = tensor[..., :half]
    second = tensor[..., half:]
    return jnp.concatenate([first * cos_t - second * sin_t, second * cos_t + first * sin_t], axis=-1)


def rms_norm(tensor, gain):
    vec_f32 = tensor.astype(jnp.float32)
    inv_rms = lax.rsqrt(jnp.mean(vec_f32 * vec_f32, axis=-1, keepdims=True) + NORM_EPS)
    return (vec_f32 * inv_rms * gain.astype(jnp.float32)).astype(jnp.bfloat16)


def project_rows(rows, pos_rows, attn_gain, w_q, w_k, w_v):
    count = rows.shape[0]
    normed = rms_norm(rows, attn_gain)
    angles = pos_rows.astype(jnp.float32)[:, None] * rope_freqs()[None, :]
    cos_t = jnp.cos(angles)[:, None, :]
    sin_t = jnp.sin(angles)[:, None, :]
    q_raw = jnp.dot(normed, w_q, preferred_element_type=jnp.float32).reshape(count, HEADS, HEAD_DIM)
    k_raw = jnp.dot(normed, w_k, preferred_element_type=jnp.float32).reshape(count, KV_HEADS, HEAD_DIM)
    v_raw = jnp.dot(normed, w_v, preferred_element_type=jnp.float32).reshape(count, KV_HEADS, HEAD_DIM)
    q_heads = apply_rope(q_raw, cos_t, sin_t).astype(jnp.bfloat16)
    k_heads = apply_rope(k_raw, cos_t, sin_t).astype(jnp.bfloat16)
    return q_heads, k_heads, v_raw.astype(jnp.bfloat16)


def attend_rows(block, k_all, v_all, seg_ids, positions):
    q_block, seg_rows, pos_rows = block
    q_grp = q_block.astype(jnp.float32).reshape(ATT_ROWS, KV_HEADS, GROUP_REP, HEAD_DIM)
    scores = jnp.einsum('qgrd,sgd->grqs', q_grp, k_all) * (HEAD_DIM ** -0.5)
    visible = (seg_ids[None, :] == seg_rows[:, None]) & (positions[None, :] <= pos_rows[:, None])
    scores = jnp.where(visible[None, None], scores, NEG_BIG)
    prob_w = jax.nn.softmax(scores, axis=-1)
    out_rows = jnp.einsum('grqs,sgd->qgrd', prob_w, v_all)
    return out_rows.reshape(ATT_ROWS, HEADS * HEAD_DIM).astype(jnp.bfloat16)


def finish_rows(rows, attn_rows, w_o, mlp_gain, w_gate, w_up, w_down):
    resid_mid = (rows.astype(jnp.float32) + jnp.dot(attn_rows, w_o, preferred_element_type=jnp.float32)).astype(jnp.bfloat16)
    normed = rms_norm(resid_mid, mlp_gain)
    gate = jnp.dot(normed, w_gate, preferred_element_type=jnp.float32)
    up_val = jnp.dot(normed, w_up, preferred_element_type=jnp.float32)
    hidden = (jax.nn.silu(gate) * up_val).astype(jnp.bfloat16)
    return (resid_mid.astype(jnp.float32) + jnp.dot(hidden, w_down, preferred_element_type=jnp.float32)).astype(jnp.bfloat16)


def mirror_order():
    row_idx = jnp.arange(SEQ_LEN)
    device = row_idx // TOKENS_DEV
    within = row_idx % TOKENS_DEV
    chunk_id = jnp.where(within < CHUNK_ROWS, device, 2 * CP_SIZE - 1 - device)
    return chunk_id * CHUNK_ROWS + within % CHUNK_ROWS


def draw_layout(key):
    key_long, key_cuts = jax.random.split(key)
    long_len = SEQ_LEN // 2 + jax.random.randint(key_long, (), 0, SEQ_LEN // 4 + 1)
    cuts = jnp.sort(jax.random.randint(key_cuts, (NUM_PROMPTS - 2,), long_len, SEQ_LEN))
    bounds = jnp.concatenate([long_len[None], cuts]).astype(jnp.int32)
    token = jnp.arange(SEQ_LEN, dtype=jnp.int32)
    after = token[:, None] >= bounds[None, :]
    seg_nat = jnp.sum(after, axis=1).astype(jnp.int32)
    start = jnp.max(jnp.where(after, bounds[None, :], 0), axis=1)
    pos_nat = (token - start).astype(jnp.int32)
    order = mirror_order()
    return seg_nat[order], pos_nat[order]


def normal_weight(key, shape, scale):
    return (scale * jax.random.normal(key, shape, jnp.float32)).astype(jnp.bfloat16)


def setup_inputs(seed: int = 0, part: int = 0) -> dict:
    root = jax.random.key(seed)
    shared = jax.random.split(root, 10)
    part_keys = jax.random.split(jax.random.fold_in(root, part), 2)
    seg_ids, positions = draw_layout(part_keys[0])
    x_in = normal_weight(part_keys[1], (1, SEQ_LEN, MODEL_DIM), 0.5)
    attn_gain = (1.0 + 0.3 * jax.random.normal(shared[0], (MODEL_DIM,), jnp.float32)).astype(jnp.bfloat16)
    w_q = normal_weight(shared[1], (MODEL_DIM, HEADS * HEAD_DIM), 1.5 * MODEL_DIM ** -0.5)
    w_k = normal_weight(shared[2], (MODEL_DIM, KV_HEADS * HEAD_DIM), 1.5 * MODEL_DIM ** -0.5)
    w_v = normal_weight(shared[3], (MODEL_DIM, KV_HEADS * HEAD_DIM), MODEL_DIM ** -0.5)
    w_o = normal_weight(shared[4], (HEADS * HEAD_DIM, MODEL_DIM), 2.0 * (HEADS * HEAD_DIM) ** -0.5)
    mlp_gain = (1.0 + 0.3 * jax.random.normal(shared[5], (MODEL_DIM,), jnp.float32)).astype(jnp.bfloat16)
    w_gate = normal_weight(shared[6], (MODEL_DIM, FF_DIM), MODEL_DIM ** -0.5)
    w_up = normal_weight(shared[7], (MODEL_DIM, FF_DIM), MODEL_DIM ** -0.5)
    w_down = normal_weight(shared[8], (FF_DIM, MODEL_DIM), FF_DIM ** -0.5)
    return {'x_in': x_in, 'seg_ids': seg_ids, 'positions': positions, 'attn_gain': attn_gain, 'w_q': w_q, 'w_k': w_k, 'w_v': w_v, 'w_o': w_o, 'mlp_gain': mlp_gain, 'w_gate': w_gate, 'w_up': w_up, 'w_down': w_down}


def reference(x_in, seg_ids, positions, attn_gain, w_q, w_k, w_v, w_o, mlp_gain, w_gate, w_up, w_down):
    num_blocks = SEQ_LEN // CHUNK_ROWS
    row_blocks = x_in.reshape(num_blocks, CHUNK_ROWS, MODEL_DIM)
    pos_blocks = positions.reshape(num_blocks, CHUNK_ROWS)
    q_heads, k_heads, v_heads = lax.map(lambda block: project_rows(block[0], block[1], attn_gain, w_q, w_k, w_v), (row_blocks, pos_blocks))
    k_cache = k_heads.reshape(SEQ_LEN, KV_HEADS, HEAD_DIM)
    v_cache = v_heads.reshape(SEQ_LEN, KV_HEADS, HEAD_DIM)
    k_all = k_cache.astype(jnp.float32)
    v_all = v_cache.astype(jnp.float32)
    q_rows = q_heads.reshape(SEQ_LEN // ATT_ROWS, ATT_ROWS, HEADS, HEAD_DIM)
    seg_rows = seg_ids.reshape(SEQ_LEN // ATT_ROWS, ATT_ROWS)
    pos_rows = positions.reshape(SEQ_LEN // ATT_ROWS, ATT_ROWS)
    attn_rows = lax.map(lambda block: attend_rows(block, k_all, v_all, seg_ids, positions), (q_rows, seg_rows, pos_rows))
    attn_blocks = attn_rows.reshape(num_blocks, CHUNK_ROWS, HEADS * HEAD_DIM)
    z_blocks = lax.map(lambda block: finish_rows(block[0], block[1], w_o, mlp_gain, w_gate, w_up, w_down), (row_blocks, attn_blocks))
    return z_blocks.reshape(1, SEQ_LEN, MODEL_DIM), k_cache, v_cache
```

```python
import functools
import math

import jax
import jax.numpy as jnp
from jax import lax
from jax.experimental import pallas as pl
from jax.experimental.pallas import tpu as pltpu
from jax.sharding import PartitionSpec as P

HEAD_DIM = 128
ROPE_THETA = 500000.0
ROPE_FACTOR = 8.0
LOW_FREQ = 1.0
HIGH_FREQ = 4.0
ORIG_CTX = 8192.0
NORM_EPS = 1e-5
NEG_BIG = -1e30
SCORE_LOG2 = HEAD_DIM ** -0.5 * math.log2(math.e)
MESH = pl.DeviceIdType.MESH
COLS = 512
SLOTS = 10
OWNERS = 4
LANES = 256
F32 = jnp.float32
BF16 = jnp.bfloat16


def rope_freqs():
    exponent = jnp.arange(0, HEAD_DIM, 2).astype(F32) / HEAD_DIM
    inv_freq = 1.0 / (ROPE_THETA ** exponent)
    wavelen = 2.0 * jnp.pi / inv_freq
    smooth = jnp.clip((ORIG_CTX / wavelen - LOW_FREQ) / (HIGH_FREQ - LOW_FREQ), 0.0, 1.0)
    return (1.0 - smooth) * inv_freq / ROPE_FACTOR + smooth * inv_freq


def fdot(lhs, rhs):
    return jnp.dot(lhs, rhs, preferred_element_type=F32)


def norm_rows(src_ref, dst_ref, gain_ref, row, count):
    depth = src_ref.shape[1]
    rows = pl.ds(row, count)
    total = jnp.zeros((count, 128), F32)
    for col in range(0, depth, 128):
        part = src_ref[rows, col:col + 128].astype(F32)
        total = total + part * part
    inv_rms = lax.rsqrt(jnp.sum(total, axis=1, keepdims=True) / depth + NORM_EPS)
    for col in range(0, depth, 512):
        part = src_ref[rows, col:col + 512].astype(F32)
        gain = gain_ref[:, col:col + 512].astype(F32)
        dst_ref[rows, col:col + 512] = (part * inv_rms * gain).astype(BF16)


def project_kernel(x_hbm, gain_ref, cos_ref, sin_ref, wq_hbm, wk_hbm, wv_hbm, qt_ref, kv_ref, kc_ref, vc_ref, x_buf, a_buf, wkv_buf, wq_buf, x_sem, wkv_sem, wq_sem):
    count, depth = x_buf.shape
    piece = count // 2
    heads = wq_hbm.shape[1] // HEAD_DIM
    half_depth = depth // 2
    blocks = x_sem.shape[0]
    rows_blk = count // blocks

    def x_copy(idx):
        rows = pl.ds(idx * rows_blk, rows_blk)
        return pltpu.make_async_copy(x_hbm.at[rows], x_buf.at[rows], x_sem.at[idx])

    for idx in range(blocks):
        x_copy(idx).start()
    wkv = [pltpu.make_async_copy(src, wkv_buf.at[:, idx * HEAD_DIM:(idx + 1) * HEAD_DIM], wkv_sem.at[idx]) for idx, src in enumerate((wk_hbm, wv_hbm))]
    for copy in wkv:
        copy.start()
    wq_copies = []
    for col in range(wq_hbm.shape[1] // COLS):
        for part in range(2):
            slot = 2 * col + part
            copy = pltpu.make_async_copy(wq_hbm.at[pl.ds(part * half_depth, half_depth), pl.ds(col * COLS, COLS)], wq_buf.at[slot], wq_sem.at[slot])
            copy.start()
            wq_copies.append(copy)

    @pl.loop(0, blocks)
    def _(idx):
        x_copy(idx).wait()
        norm_rows(x_buf, a_buf, gain_ref, pl.multiple_of(idx * rows_blk, rows_blk), rows_blk)

    for copy in wkv:
        copy.wait()
    kv_raw = fdot(a_buf[...], wkv_buf[...])
    cos_t = cos_ref[...]
    sin_t = sin_ref[...]

    def rope(raw):
        return raw * cos_t + pltpu.roll(raw, HEAD_DIM // 2, 1) * sin_t

    k_rot = rope(kv_raw[:, :HEAD_DIM])
    v_raw = kv_raw[:, HEAD_DIM:]
    kc_ref[...] = k_rot.astype(BF16)
    vc_ref[...] = v_raw.astype(BF16)
    for half in range(2):
        rows = slice(half * piece, (half + 1) * piece)
        kv_ref[half] = k_rot[rows].astype(BF16)
        kv_ref[2 + half] = v_raw[rows].T.astype(BF16)

    for col in range(wq_hbm.shape[1] // COLS):
        wq_copies[2 * col].wait()
        wq_copies[2 * col + 1].wait()
        q_raw = fdot(a_buf[:, :half_depth], wq_buf[2 * col]) + fdot(a_buf[:, half_depth:], wq_buf[2 * col + 1])
        for sub in range(COLS // HEAD_DIM):
            head = col * (COLS // HEAD_DIM) + sub
            q_rot = rope(q_raw[:, sub * HEAD_DIM:(sub + 1) * HEAD_DIM])
            for half in range(2):
                qt_ref[half, :, head * piece:(head + 1) * piece] = q_rot[half * piece:(half + 1) * piece].T.astype(BF16)


def gather_shards(side, kv_ref, all_ref, send_sem, recv_sem):
    me = lax.axis_index('cp')
    core = lax.rem(me, 2)
    chip = me // 2
    chip_x = lax.rem(chip, side)
    chip_y = chip // side

    def owner(first, second):
        pos_x = lax.rem(chip_x + first * (1 - core) + second * core + 2 * side, side)
        pos_y = lax.rem(chip_y + first * core + second * (1 - core) + 2 * side, side)
        return (pos_y * side + pos_x) * 2 + core

    sibling = me + 1 - 2 * core
    targets = {'a+': owner(1, 0), 'a-': owner(-1, 0), 'b+': owner(0, 1), 'b-': owner(0, -1), 's': sibling}
    barrier = pltpu.get_barrier_semaphore()
    for target in targets.values():
        pl.semaphore_signal(barrier, inc=1, device_id={'cp': target}, device_id_type=MESH)
    pl.semaphore_wait(barrier, len(targets))

    copies = []

    def send(shard, where, half=None):
        num = len(copies)
        dst = all_ref.at[shard]
        src = kv_ref if num < 5 else dst
        if half is not None:
            dst = dst.at[pl.ds(2 * half, 2)]
            src = dst
        copy = pltpu.make_async_remote_copy(src_ref=src, dst_ref=dst, send_sem=send_sem.at[num], recv_sem=recv_sem.at[num], device_id={'cp': targets[where]}, device_id_type=MESH)
        copy.start()
        copies.append(copy)
        return copy

    from_sibling = []

    def spread(shard):
        plus = send(shard, 'b+')
        minus = send(shard, 'b-')
        from_sibling.append(send(shard, 's'))
        return plus, minus

    own_right = send(me, 'a+')
    own_left = send(me, 'a-')
    row_own = spread(me)
    all_ref[me] = kv_ref[...]
    own_right.wait_recv()
    shard = owner(-1, 0)
    far_k = send(shard, 'a+', 0)
    row_left = spread(shard)
    own_left.wait_recv()
    shard = owner(1, 0)
    far_v = send(shard, 'a-', 1)
    row_right = spread(shard)

    def relay(first, row):
        row[0].wait_recv()
        shard = owner(first, -1)
        half_k = send(shard, 'b+', 0)
        from_sibling.append(send(shard, 's'))
        row[1].wait_recv()
        shard = owner(first, 1)
        half_v = send(shard, 'b-', 1)
        from_sibling.append(send(shard, 's'))
        return half_k, half_v

    def close(first, halves):
        halves[0].wait_recv()
        halves[1].wait_recv()
        from_sibling.append(send(owner(first, 2), 's'))

    far_own = relay(0, row_own)
    far_k.wait_recv()
    far_v.wait_recv()
    row_far = spread(owner(2, 0))
    far_left = relay(-1, row_left)
    far_right = relay(1, row_right)
    close(0, far_own)
    far_far = relay(2, row_far)
    close(-1, far_left)
    close(1, far_right)
    close(2, far_far)
    for copy in from_sibling:
        copy.wait_recv()
    for copy in copies:
        copy.wait_send()


NUM_COPIES = 36


def attend_kernel(cp_size, side, kv_ref, qt_ref, pos_ref, out_ref, all_ref, max_ref, sum_ref, acc_ref, send_sem, recv_sem):
    gather_shards(side, kv_ref, all_ref, send_sem, recv_sem)
    me = lax.axis_index('cp')
    piece = kv_ref.shape[1]
    width = qt_ref.shape[2]
    tiles = width // LANES
    bases = (me * piece, (2 * cp_size - 1 - me) * piece)
    lane_tok = lax.broadcasted_iota(jnp.int32, (1, piece), 1)

    def starts(half):
        first = bases[half] + lane_tok - pos_ref[half]
        return jnp.concatenate([first] * (LANES // piece), axis=1)

    first_key = (starts(0), starts(1))
    tok = jnp.concatenate([lane_tok] * (LANES // piece), axis=1)
    key_row = lax.broadcasted_iota(jnp.int32, (piece, LANES), 0)

    for half in range(2):
        visible = (key_row <= tok) & (key_row + bases[half] >= first_key[half])
        for tile in range(tiles):
            cols = slice(tile * LANES, (tile + 1) * LANES)
            scores = fdot(kv_ref[half], qt_ref[half, :, cols])
            scores = jnp.where(visible, scores, NEG_BIG)
            top = jnp.max(scores, axis=0, keepdims=True)
            prob = jnp.exp2((scores - top) * SCORE_LOG2)
            max_ref[half, :, cols] = top
            sum_ref[half, :, cols] = jnp.sum(prob, axis=0, keepdims=True)
            acc_ref[half, :, cols] = fdot(kv_ref[2 + half], prob.astype(BF16))

    def chunk(half, part, idx):
        first = idx * OWNERS
        key_base = []
        for sub in range(OWNERS):
            own = first + sub
            if part == 0:
                base = own * piece
                base = base if half == 1 else jnp.where(own < me, base, -2 * piece)
            else:
                base = jnp.where(own > me, (2 * cp_size - 1 - own) * piece, -2 * piece)
            key_base.append(base)
        keys = all_ref[pl.ds(first, OWNERS), part].reshape(OWNERS * piece, HEAD_DIM)
        vals = jnp.concatenate([all_ref[first + sub, 2 + part] for sub in range(OWNERS)], axis=1)
        for tile in range(tiles):
            cols = slice(tile * LANES, (tile + 1) * LANES)
            raw = fdot(keys, qt_ref[half, :, cols])
            scores = [jnp.where(key_row >= first_key[half] - key_base[sub], raw[sub * piece:(sub + 1) * piece], NEG_BIG) for sub in range(OWNERS)]
            old_top = max_ref[half, :, cols]
            peak = functools.reduce(jnp.maximum, scores)
            top = jnp.maximum(old_top, jnp.max(peak, axis=0, keepdims=True))
            probs = [jnp.exp2((score - top) * SCORE_LOG2) for score in scores]
            scale = jnp.exp2((old_top - top) * SCORE_LOG2)
            max_ref[half, :, cols] = top
            sum_ref[half, :, cols] = sum_ref[half, :, cols] * scale + jnp.sum(functools.reduce(jnp.add, probs), axis=0, keepdims=True)
            prob = jnp.concatenate([part_p.astype(BF16) for part_p in probs], axis=0)
            acc_ref[half, :, cols] = acc_ref[half, :, cols] * scale + fdot(vals, prob)

    @pl.loop(0, cp_size // OWNERS)
    def _(idx):
        chunk(1, 0, idx)

    @pl.loop(0, (me + OWNERS - 1) // OWNERS)
    def _(idx):
        chunk(0, 0, idx)

    @pl.loop((me + 1) // OWNERS, cp_size // OWNERS)
    def _(idx):
        chunk(1, 1, idx)

    for half in range(2):
        for head in range(width // piece):
            cols = slice(head * piece, (head + 1) * piece)
            done = acc_ref[half, :, cols] / sum_ref[half, :, cols]
            out_ref[half * piece:(half + 1) * piece, head * HEAD_DIM:(head + 1) * HEAD_DIM] = done.T.astype(BF16)


def finish_kernel(x_hbm, attn_ref, gain_ref, wo_hbm, wg_hbm, wu_hbm, wd_hbm, z_hbm, h_buf, b_buf, m_buf, z_buf, slots, x_sem, slot_sem, z_sem):
    count, depth = h_buf.shape
    slot_rows = slots.shape[1]
    attn_w = attn_ref.shape[1]
    stack = slot_rows // attn_w
    ff = wg_hbm.shape[1]
    n_wo = depth // COLS // stack
    n_ff = ff // COLS
    n_dn = depth // COLS
    up_from = n_wo
    dn_from = n_wo + 4 * n_ff
    total = dn_from + n_dn

    def col(idx):
        return pl.ds(pl.multiple_of(idx * COLS, COLS), COLS)

    def issue(num):
        slot = lax.rem(num, SLOTS)
        sem = slot_sem.at[slot]

        @pl.when(num < up_from)
        def _():
            for sub in range(stack):
                pltpu.make_async_copy(wo_hbm.at[:, col(num * stack + sub)], slots.at[slot, pl.ds(sub * attn_w, attn_w)], sem).start()

        rel = num - up_from
        blk = rel // 4
        kind = lax.rem(rel, 4)
        rows = pl.ds(pl.multiple_of(lax.rem(kind, 2) * slot_rows, slot_rows), slot_rows)

        @pl.when((num >= up_from) & (num < dn_from) & (kind < 2))
        def _():
            pltpu.make_async_copy(wg_hbm.at[rows, col(blk)], slots.at[slot], sem).start()

        @pl.when((num >= up_from) & (num < dn_from) & (kind >= 2))
        def _():
            pltpu.make_async_copy(wu_hbm.at[rows, col(blk)], slots.at[slot], sem).start()

        @pl.when((num >= dn_from) & (num < total))
        def _():
            pltpu.make_async_copy(wd_hbm.at[:, col(num - dn_from)], slots.at[slot, pl.ds(0, ff)], sem).start()

    def take(num, rows):
        slot = lax.rem(num, SLOTS)
        part = slots.at[slot, pl.ds(0, rows)]
        pltpu.make_async_copy(part, part, slot_sem.at[slot]).wait()
        return slots.at[slot]

    x_copy = pltpu.make_async_copy(x_hbm, h_buf, x_sem)
    x_copy.start()
    for num in range(SLOTS):
        issue(jnp.int32(num))
    x_copy.wait()

    @pl.loop(0, n_wo)
    def _(num):
        slot = take(num, slot_rows)
        for sub in range(stack):
            cols = col(num * stack + sub)
            out = fdot(attn_ref[...], slot[sub * attn_w:(sub + 1) * attn_w])
            h_buf[:, cols] = (h_buf[:, cols].astype(F32) + out).astype(BF16)
        issue(num + SLOTS)

    @pl.loop(0, count // 32)
    def _(idx):
        norm_rows(h_buf, b_buf, gain_ref, pl.multiple_of(idx * 32, 32), 32)

    @pl.loop(0, n_ff)
    def _(blk):
        first = up_from + 4 * blk

        def product(num):
            low = take(num, slot_rows)
            res = fdot(b_buf[:, :slot_rows], low[...])
            high = take(num + 1, slot_rows)
            return res + fdot(b_buf[:, slot_rows:], high[...])

        gate = product(first)
        issue(first + SLOTS)
        issue(first + 1 + SLOTS)
        up_val = product(first + 2)
        issue(first + 2 + SLOTS)
        issue(first + 3 + SLOTS)
        m_buf[:, col(blk)] = (gate * jax.nn.sigmoid(gate) * up_val).astype(BF16)

    def z_copy(blk):
        slot = lax.rem(blk, 2)
        return pltpu.make_async_copy(z_buf.at[slot], z_hbm.at[:, col(blk)], z_sem.at[slot])

    @pl.loop(0, n_dn)
    def _(blk):
        num = dn_from + blk
        slot = take(num, ff)
        out = fdot(m_buf[...], slot[:ff])

        @pl.when(blk >= 2)
        def _():
            z_copy(blk - 2).wait()

        z_buf[lax.rem(blk, 2)] = (h_buf[:, col(blk)].astype(F32) + out).astype(BF16)
        z_copy(blk).start()
        issue(num + SLOTS)

    z_copy(n_dn - 2).wait()
    z_copy(n_dn - 1).wait()


def solution(mesh):
    cp_size = mesh.shape['cp']
    side = math.isqrt(cp_size // 2)
    vmem = pl.BlockSpec(memory_space=pltpu.VMEM)
    hbm = pl.BlockSpec(memory_space=pl.ANY)
    dma = pltpu.SemaphoreType.DMA
    limit = 60 * 1024 * 1024

    def device_fn(x_loc, seg_loc, pos_loc, attn_gain, w_q, w_k, w_v, w_o, mlp_gain, w_gate, w_up, w_down):
        rows = x_loc[0]
        count, depth = rows.shape
        piece = count // 2
        width = w_q.shape[1] // HEAD_DIM * piece
        ff = w_gate.shape[1]
        angles = pos_loc.astype(F32)[:, None] * rope_freqs()[None, :]
        cos_t = jnp.cos(angles)
        sin_t = jnp.sin(angles)
        cos_t = jnp.concatenate([cos_t, cos_t], axis=1)
        sin_t = jnp.concatenate([-sin_t, sin_t], axis=1)
        q_t, kv, k_rows, v_rows = pl.pallas_call(
            project_kernel,
            out_shape=(jax.ShapeDtypeStruct((2, HEAD_DIM, width), BF16), jax.ShapeDtypeStruct((4, piece, HEAD_DIM), BF16), jax.ShapeDtypeStruct((count, HEAD_DIM), BF16), jax.ShapeDtypeStruct((count, HEAD_DIM), BF16)),
            in_specs=[hbm, vmem, vmem, vmem, hbm, hbm, hbm],
            out_specs=(vmem, vmem, vmem, vmem),
            scratch_shapes=[pltpu.VMEM((count, depth), BF16), pltpu.VMEM((count, depth), BF16), pltpu.VMEM((depth, 2 * HEAD_DIM), BF16), pltpu.VMEM((2 * w_q.shape[1] // COLS, depth // 2, COLS), BF16), dma((count // 32,)), dma((2,)), dma((2 * w_q.shape[1] // COLS,))],
            compiler_params=pltpu.CompilerParams(vmem_limit_bytes=limit),
            name='project',
        )(rows, attn_gain.reshape(1, depth), cos_t, sin_t, w_q, w_k, w_v)
        attn_rows = pl.pallas_call(
            functools.partial(attend_kernel, cp_size, side),
            out_shape=jax.ShapeDtypeStruct((count, w_q.shape[1]), BF16),
            in_specs=[vmem, vmem, vmem],
            out_specs=vmem,
            scratch_shapes=[pltpu.VMEM((cp_size, 4, piece, HEAD_DIM), BF16), pltpu.VMEM((2, 1, width), F32), pltpu.VMEM((2, 1, width), F32), pltpu.VMEM((2, HEAD_DIM, width), F32), dma((NUM_COPIES,)), dma((NUM_COPIES,))],
            compiler_params=pltpu.CompilerParams(vmem_limit_bytes=limit, collective_id=0, has_side_effects=True),
            name='attend',
        )(kv, q_t, pos_loc.reshape(2, 1, piece))
        z_rows = pl.pallas_call(
            finish_kernel,
            out_shape=jax.ShapeDtypeStruct((count, depth), BF16),
            in_specs=[hbm, vmem, vmem, hbm, hbm, hbm, hbm],
            out_specs=hbm,
            scratch_shapes=[pltpu.VMEM((count, depth), BF16), pltpu.VMEM((count, depth), BF16), pltpu.VMEM((count, ff), BF16), pltpu.VMEM((2, count, COLS), BF16), pltpu.VMEM((SLOTS, depth // 2, COLS), BF16), dma(()), dma((SLOTS,)), dma((2,))],
            compiler_params=pltpu.CompilerParams(vmem_limit_bytes=limit),
            name='finish',
        )(rows, attn_rows, mlp_gain.reshape(1, depth), w_o, w_gate, w_up, w_down)
        return z_rows[None], k_rows[:, None, :], v_rows[:, None, :]

    seq_spec = P(('dp', 'cp'))
    return jax.shard_map(device_fn, mesh=mesh, in_specs=(P('dp', 'cp', None), seq_spec, seq_spec, P(), P(), P(), P(), P(), P(), P(), P(), P()), out_specs=(P('dp', 'cp', None), P(('dp', 'cp'), None, None), P(('dp', 'cp'), None, None)), check_vma=False)
```

```python
import functools
import math

import jax
import jax.numpy as jnp
import numpy as np
from jax import lax
from jax.experimental import pallas as pl
from jax.experimental.pallas import tpu as pltpu
from jax.sharding import PartitionSpec as P

HEAD_DIM = 128
ROPE_THETA = 500000.0
ROPE_FACTOR = 8.0
LOW_FREQ = 1.0
HIGH_FREQ = 4.0
ORIG_CTX = 8192.0
NORM_EPS = 1e-5
NEG_BIG = -1e30
SCORE_LOG2 = HEAD_DIM ** -0.5 * math.log2(math.e)
MESH = pl.DeviceIdType.MESH
COLS = 512
SLOTS = 8
SLOT_ROWS = 1024
SLOT_COLS = 2048
OWNERS = 4
LANES = 256
F32 = jnp.float32
BF16 = jnp.bfloat16


def rope_freqs():
    exponent = np.arange(0, HEAD_DIM, 2) / HEAD_DIM
    inv_freq = 1.0 / (ROPE_THETA ** exponent)
    wavelen = 2.0 * np.pi / inv_freq
    smooth = np.clip((ORIG_CTX / wavelen - LOW_FREQ) / (HIGH_FREQ - LOW_FREQ), 0.0, 1.0)
    return ((1.0 - smooth) * inv_freq / ROPE_FACTOR + smooth * inv_freq).astype(np.float32)


def fdot(lhs, rhs):
    return jnp.dot(lhs, rhs, preferred_element_type=F32)


def norm_rows(src_ref, dst_ref, gain_ref, row, count):
    depth = src_ref.shape[1]
    rows = pl.ds(row, count)
    total = jnp.zeros((count, 128), F32)
    for col in range(0, depth, 128):
        part = src_ref[rows, col:col + 128].astype(F32)
        total = total + part * part
    inv_rms = lax.rsqrt(jnp.sum(total, axis=1, keepdims=True) / depth + NORM_EPS)
    for col in range(0, depth, 512):
        part = src_ref[rows, col:col + 512].astype(F32)
        gain = gain_ref[col:col + 512].astype(F32).reshape(1, 512)
        dst_ref[rows, col:col + 512] = (part * inv_rms * gain).astype(BF16)


def project_kernel(x_hbm, gain_ref, pos_ref, freq_ref, wq_hbm, wk_hbm, wv_hbm, qt_ref, kv_ref, kc_ref, vc_ref, x_buf, a_buf, wk_buf, wv_buf, wq_buf, x_sem, wkv_sem, wq_sem):
    count, depth = x_buf.shape
    piece = count // 2
    blocks = x_sem.shape[0]
    rows_blk = count // blocks
    chunks = wq_buf.shape[0]
    chunk_rows = wq_buf.shape[1]

    def x_copy(idx):
        rows = pl.ds(idx * rows_blk, rows_blk)
        return pltpu.make_async_copy(x_hbm.at[rows], x_buf.at[rows], x_sem.at[idx])

    for idx in range(blocks):
        x_copy(idx).start()
    wkv = [pltpu.make_async_copy(wk_hbm, wk_buf, wkv_sem.at[0]), pltpu.make_async_copy(wv_hbm, wv_buf, wkv_sem.at[1])]
    for copy in wkv:
        copy.start()
    wq_copies = [pltpu.make_async_copy(wq_hbm.at[pl.ds(idx * chunk_rows, chunk_rows)], wq_buf.at[idx], wq_sem.at[idx]) for idx in range(chunks)]
    for copy in wq_copies:
        copy.start()

    cos_t, sin_t = rope_tables(pos_ref, freq_ref)

    @pl.loop(0, blocks)
    def _(idx):
        x_copy(idx).wait()
        norm_rows(x_buf, a_buf, gain_ref, pl.multiple_of(idx * rows_blk, rows_blk), rows_blk)

    for copy in wkv:
        copy.wait()
    kv_raw = fdot(a_buf[...], jnp.concatenate([wk_buf[...], wv_buf[...]], axis=1))

    def rope(raw):
        return raw * cos_t + pltpu.roll(raw, HEAD_DIM // 2, 1) * sin_t

    k_rot = rope(kv_raw[:, :HEAD_DIM])
    v_raw = kv_raw[:, HEAD_DIM:]
    kc_ref[...] = k_rot.astype(BF16)
    vc_ref[...] = v_raw.astype(BF16)
    for half in range(2):
        rows = slice(half * piece, (half + 1) * piece)
        kv_ref[half] = k_rot[rows].astype(BF16)
        kv_ref[2 + half] = v_raw[rows].T.astype(BF16)

    for copy in wq_copies:
        copy.wait()
    for col in range(wq_hbm.shape[1] // COLS):
        q_raw = fdot(a_buf[...], jnp.concatenate([wq_buf[idx, :, col * COLS:(col + 1) * COLS] for idx in range(chunks)], axis=0))
        for sub in range(COLS // HEAD_DIM):
            head = col * (COLS // HEAD_DIM) + sub
            q_rot = rope(q_raw[:, sub * HEAD_DIM:(sub + 1) * HEAD_DIM])
            for half in range(2):
                qt_ref[half, :, head * piece:(head + 1) * piece] = q_rot[half * piece:(half + 1) * piece].T.astype(BF16)


def rope_tables(pos_ref, freq_ref):
    cos_parts, sin_parts = [], []
    for half in range(2):
        angles = freq_ref[...] * pos_ref[half].astype(F32)
        cos_parts.append(jnp.cos(angles).T)
        sin_parts.append(jnp.sin(angles).T)
    cos_h = jnp.concatenate(cos_parts, axis=0)
    sin_h = jnp.concatenate(sin_parts, axis=0)
    return jnp.concatenate([cos_h, cos_h], axis=1), jnp.concatenate([-sin_h, sin_h], axis=1)


def gather_shards(side, kv_ref, all_ref, send_sem, recv_sem, on_start, on_group):
    me = lax.axis_index('cp')
    core = lax.rem(me, 2)
    chip = me // 2
    chip_x = lax.rem(chip, side)
    chip_y = chip // side

    def owner(first, second, core=core):
        pos_x = lax.rem(chip_x + first * (1 - core) + second * core + 2 * side, side)
        pos_y = lax.rem(chip_y + first * core + second * (1 - core) + 2 * side, side)
        return (pos_y * side + pos_x) * 2 + core

    def other(first, second):
        return owner(first, second, 1 - core)

    sibling = me + 1 - 2 * core
    targets = {'a+': owner(1, 0), 'a-': owner(-1, 0), 'b+': owner(0, 1), 'b-': owner(0, -1), 's': sibling}
    barrier = pltpu.get_barrier_semaphore()
    for target in targets.values():
        pl.semaphore_signal(barrier, inc=1, device_id={'cp': target}, device_id_type=MESH)
    pl.semaphore_wait(barrier, len(targets))

    copies = []

    def send(shard, where, half=None):
        num = len(copies)
        dst = all_ref.at[shard]
        src = kv_ref if num < 5 else dst
        if half is not None:
            dst = dst.at[pl.ds(2 * half, 2)]
            src = dst
        copy = pltpu.make_async_remote_copy(src_ref=src, dst_ref=dst, send_sem=send_sem.at[num], recv_sem=recv_sem.at[num], device_id={'cp': targets[where]}, device_id_type=MESH)
        copy.start()
        copies.append(copy)
        return copy

    from_sibling = []

    def spread(shard):
        plus = send(shard, 'b+')
        minus = send(shard, 'b-')
        from_sibling.append(send(shard, 's'))
        return plus, minus

    own_right = send(me, 'a+')
    own_left = send(me, 'a-')
    row_own = spread(me)
    all_ref[me] = kv_ref[...]
    on_start()
    own_right.wait_recv()
    shard = owner(-1, 0)
    far_k = send(shard, 'a+', 0)
    row_left = spread(shard)
    own_left.wait_recv()
    shard = owner(1, 0)
    far_v = send(shard, 'a-', 1)
    row_right = spread(shard)

    def relay(first, row):
        row[0].wait_recv()
        shard = owner(first, -1)
        half_k = send(shard, 'b+', 0)
        from_sibling.append(send(shard, 's'))
        row[1].wait_recv()
        shard = owner(first, 1)
        half_v = send(shard, 'b-', 1)
        from_sibling.append(send(shard, 's'))
        return half_k, half_v

    def close(first, halves):
        halves[0].wait_recv()
        halves[1].wait_recv()
        from_sibling.append(send(owner(first, 2), 's'))

    def arrived(*nums):
        for num in nums:
            from_sibling[num].wait_recv()

    arrived(0)
    on_group(me, sibling, owner(-1, 0), owner(1, 0))
    far_own = relay(0, row_own)
    far_k.wait_recv()
    far_v.wait_recv()
    row_far = spread(owner(2, 0))
    arrived(1, 2)
    on_group(owner(0, -1), owner(0, 1), other(-1, 0), other(1, 0))
    far_left = relay(-1, row_left)
    far_right = relay(1, row_right)
    arrived(3, 4)
    on_group(owner(2, 0), owner(-1, -1), other(0, -1), other(0, 1))
    close(0, far_own)
    far_far = relay(2, row_far)
    arrived(5)
    on_group(owner(-1, 1), owner(1, -1), owner(1, 1), other(2, 0))
    close(-1, far_left)
    close(1, far_right)
    arrived(6, 7)
    on_group(owner(0, 2), owner(2, -1), other(-1, -1), other(-1, 1))
    close(2, far_far)
    arrived(8, 9)
    on_group(owner(2, 1), owner(-1, 2), other(1, -1), other(1, 1))
    arrived(10, 11)
    on_group(owner(1, 2), owner(2, 2), other(0, 2), other(2, -1))
    arrived(12, 13, 14, 15)
    on_group(other(2, 1), other(-1, 2), other(1, 2), other(2, 2))
    for copy in copies:
        copy.wait_send()


NUM_COPIES = 36


def attend_kernel(cp_size, side, kv_ref, qt_ref, pos_ref, out_ref, all_ref, max_ref, sum_ref, acc_ref, score_ref, send_sem, recv_sem):
    me = lax.axis_index('cp')
    piece = kv_ref.shape[1]
    width = qt_ref.shape[2]
    tiles = width // LANES
    bases = (me * piece, (2 * cp_size - 1 - me) * piece)
    lane_tok = lax.broadcasted_iota(jnp.int32, (1, piece), 1)

    def starts(half):
        first = bases[half] + lane_tok - pos_ref[half]
        return jnp.concatenate([first] * (LANES // piece), axis=1)

    first_key = (starts(0), starts(1))
    tok = jnp.concatenate([lane_tok] * (LANES // piece), axis=1)
    key_row = lax.broadcasted_iota(jnp.int32, (piece, LANES), 0)

    def diagonal():
        for half in range(2):
            visible = (key_row <= tok) & (key_row + bases[half] >= first_key[half])
            for tile in range(tiles):
                cols = slice(tile * LANES, (tile + 1) * LANES)
                scores = fdot(kv_ref[half], qt_ref[half, :, cols])
                scores = jnp.where(visible, scores, NEG_BIG)
                top = jnp.max(scores, axis=0, keepdims=True)
                prob = jnp.exp2((scores - top) * SCORE_LOG2)
                max_ref[half, :, cols] = top
                sum_ref[half, :, cols] = jnp.sum(prob, axis=0, keepdims=True)
                acc_ref[half, :, cols] = fdot(kv_ref[2 + half], prob.astype(BF16))

    def block(half, part, owners, key_base):
        keys = jnp.concatenate([all_ref[own, part] for own in owners], axis=0)
        vals = jnp.concatenate([all_ref[own, 2 + part] for own in owners], axis=1)
        hidden = [key_row < first_key[half] - base for base in key_base]
        tops, scales = [], []
        for tile in range(tiles):
            cols = slice(tile * LANES, (tile + 1) * LANES)
            raw = fdot(keys, qt_ref[half, :, cols])
            peak = None
            for sub in range(OWNERS):
                rows = slice(sub * piece, (sub + 1) * piece)
                score = jnp.where(hidden[sub], NEG_BIG, raw[rows])
                score_ref[rows, cols] = score
                best = jnp.max(score, axis=0, keepdims=True)
                peak = best if peak is None else jnp.maximum(peak, best)
            old_top = max_ref[half, :, cols]
            top = jnp.maximum(old_top, peak)
            max_ref[half, :, cols] = top
            tops.append(top)
            scales.append(jnp.exp2((old_top - top) * SCORE_LOG2))
        for tile in range(tiles):
            cols = slice(tile * LANES, (tile + 1) * LANES)
            prob = jnp.exp2((score_ref[:, cols] - tops[tile]) * SCORE_LOG2)
            sum_ref[half, :, cols] = sum_ref[half, :, cols] * scales[tile] + jnp.sum(prob, axis=0, keepdims=True)
            acc_ref[half, :, cols] = acc_ref[half, :, cols] * scales[tile] + fdot(vals, prob.astype(BF16))

    def low_group(*owners):
        block(1, 0, owners, [own * piece for own in owners])

    gather_shards(side, kv_ref, all_ref, send_sem, recv_sem, diagonal, low_group)

    @pl.loop(0, (me + OWNERS - 1) // OWNERS)
    def _(idx):
        owners = [idx * OWNERS + sub for sub in range(OWNERS)]
        block(0, 0, owners, [jnp.where(own < me, own * piece, -2 * piece) for own in owners])

    @pl.loop((me + 1) // OWNERS, cp_size // OWNERS)
    def _(idx):
        owners = [idx * OWNERS + sub for sub in range(OWNERS)]
        block(1, 1, owners, [jnp.where(own > me, (2 * cp_size - 1 - own) * piece, -2 * piece) for own in owners])

    for half in range(2):
        for head in range(width // piece):
            cols = slice(head * piece, (head + 1) * piece)
            done = acc_ref[half, :, cols] / sum_ref[half, :, cols]
            out_ref[half * piece:(half + 1) * piece, head * HEAD_DIM:(head + 1) * HEAD_DIM] = done.T.astype(BF16)


def finish_kernel(x_hbm, attn_ref, gain_ref, wo_hbm, wg_hbm, wu_hbm, wd_hbm, z_hbm, h_buf, b_buf, m_buf, acc_ref, z_buf, slots, x_sem, slot_sem, z_sem):
    count, depth = h_buf.shape
    ff = wg_hbm.shape[1]
    ff_half = ff // 2
    group = 4
    n_wo = depth // SLOT_COLS
    k_steps = depth // (SLOT_ROWS * group)
    n_ff = 4 * k_steps
    dn_rows = [min(SLOT_ROWS, ff - row) for row in range(0, ff, SLOT_ROWS)]
    n_dn = depth // SLOT_COLS
    ff_from = n_wo
    dn_from = ff_from + n_ff * group
    total = dn_from + n_dn * len(dn_rows)

    def cols_of(idx, size):
        return pl.ds(pl.multiple_of(idx * size, size), size)

    def issue(num):
        slot = lax.rem(num, SLOTS)
        sem = slot_sem.at[slot]
        dst = slots.at[slot]

        @pl.when(num < ff_from)
        def _():
            pltpu.make_async_copy(wo_hbm.at[:, cols_of(num, SLOT_COLS)], dst, sem).start()

        rel = num - ff_from
        step = rel // group
        half = step // (2 * k_steps)
        kind = lax.rem(step // k_steps, 2)
        row = cols_of(lax.rem(step, k_steps) * group + lax.rem(rel, group), SLOT_ROWS)
        in_ff = (num >= ff_from) & (num < dn_from)

        @pl.when(in_ff & (kind == 0))
        def _():
            pltpu.make_async_copy(wg_hbm.at[row, cols_of(half, ff_half)], dst.at[:, pl.ds(0, ff_half)], sem).start()

        @pl.when(in_ff & (kind == 1))
        def _():
            pltpu.make_async_copy(wu_hbm.at[row, cols_of(half, ff_half)], dst.at[:, pl.ds(0, ff_half)], sem).start()

        rel = num - dn_from
        for idx, rows in enumerate(dn_rows):
            @pl.when((num >= dn_from) & (num < total) & (lax.rem(rel, len(dn_rows)) == idx))
            def _():
                src = wd_hbm.at[pl.ds(idx * SLOT_ROWS, rows), cols_of(rel // len(dn_rows), SLOT_COLS)]
                pltpu.make_async_copy(src, dst.at[pl.ds(0, rows)], sem).start()

    def take(num, rows, cols):
        slot = lax.rem(num, SLOTS)
        part = slots.at[slot, pl.ds(0, rows), pl.ds(0, cols)]
        pltpu.make_async_copy(part, part, slot_sem.at[slot]).wait()
        return slots.at[slot]

    x_copy = pltpu.make_async_copy(x_hbm, h_buf, x_sem)
    x_copy.start()
    for num in range(SLOTS):
        issue(jnp.int32(num))
    x_copy.wait()

    @pl.loop(0, n_wo)
    def _(num):
        slot = take(num, SLOT_ROWS, SLOT_COLS)
        for sub in range(0, SLOT_COLS, COLS):
            cols = pl.ds(pl.multiple_of(num * SLOT_COLS + sub, COLS), COLS)
            out = fdot(attn_ref[...], slot[:, sub:sub + COLS])
            h_buf[:, cols] = (h_buf[:, cols].astype(F32) + out).astype(BF16)
        issue(num + SLOTS)

    @pl.loop(0, count // 32)
    def _(idx):
        norm_rows(h_buf, b_buf, gain_ref, pl.multiple_of(idx * 32, 32), 32)

    @pl.loop(0, n_ff)
    def _(step):
        num = ff_from + step * group
        half = step // (2 * k_steps)
        kind = lax.rem(step // k_steps, 2)
        k_idx = lax.rem(step, k_steps)
        parts = [take(num + sub, SLOT_ROWS, ff_half) for sub in range(group)]
        lhs = b_buf[:, cols_of(k_idx, SLOT_ROWS * group)]
        for col in range(0, ff_half, COLS):
            size = min(COLS, ff_half - col)
            cols = slice(col, col + size)
            out = fdot(lhs, jnp.concatenate([part[:, cols] for part in parts], axis=0))
            acc_ref[kind, :, cols] = jnp.where(k_idx == 0, 0.0, acc_ref[kind, :, cols]) + out
        for sub in range(group):
            issue(num + sub + SLOTS)

        @pl.when((kind == 1) & (k_idx == k_steps - 1))
        def _():
            for col in range(0, ff_half, 256):
                gate = acc_ref[0, :, col:col + 256]
                dst = pl.ds(pl.multiple_of(half * ff_half + col, 256), 256)
                m_buf[:, dst] = (gate * jax.nn.sigmoid(gate) * acc_ref[1, :, col:col + 256]).astype(BF16)

    def z_copy(blk):
        slot = lax.rem(blk, 2)
        return pltpu.make_async_copy(z_buf.at[slot], z_hbm.at[:, cols_of(blk, SLOT_COLS)], z_sem.at[slot])

    @pl.loop(0, n_dn)
    def _(blk):
        num = dn_from + blk * len(dn_rows)
        parts = [take(num + idx, rows, SLOT_COLS) for idx, rows in enumerate(dn_rows)]

        @pl.when(blk >= 2)
        def _():
            z_copy(blk - 2).wait()

        for sub in range(0, SLOT_COLS, COLS):
            cols = pl.ds(pl.multiple_of(blk * SLOT_COLS + sub, COLS), COLS)
            out = fdot(m_buf[...], jnp.concatenate([part[:rows, sub:sub + COLS] for part, rows in zip(parts, dn_rows)], axis=0))
            z_buf[lax.rem(blk, 2), :, sub:sub + COLS] = (h_buf[:, cols].astype(F32) + out).astype(BF16)
        z_copy(blk).start()
        for idx in range(len(dn_rows)):
            issue(num + idx + SLOTS)

    for blk in range(max(0, n_dn - 2), n_dn):
        z_copy(blk).wait()


def solution(mesh):
    cp_size = mesh.shape['cp']
    side = math.isqrt(cp_size // 2)
    vmem = pl.BlockSpec(memory_space=pltpu.VMEM)
    hbm = pl.BlockSpec(memory_space=pl.ANY)
    dma = pltpu.SemaphoreType.DMA
    limit = 60 * 1024 * 1024

    def device_fn(x_loc, seg_loc, pos_loc, attn_gain, w_q, w_k, w_v, w_o, mlp_gain, w_gate, w_up, w_down):
        rows = x_loc[0]
        count, depth = rows.shape
        piece = count // 2
        width = w_q.shape[1] // HEAD_DIM * piece
        ff = w_gate.shape[1]
        pos3 = pos_loc.reshape(2, 1, piece)
        freqs = jnp.asarray(rope_freqs()).reshape(HEAD_DIM // 2, 1)
        q_t, kv, k_rows, v_rows = pl.pallas_call(
            project_kernel,
            out_shape=(jax.ShapeDtypeStruct((2, HEAD_DIM, width), BF16), jax.ShapeDtypeStruct((4, piece, HEAD_DIM), BF16), jax.ShapeDtypeStruct((count, HEAD_DIM), BF16), jax.ShapeDtypeStruct((count, HEAD_DIM), BF16)),
            in_specs=[hbm, vmem, vmem, vmem, hbm, hbm, hbm],
            out_specs=(vmem, vmem, vmem, vmem),
            scratch_shapes=[pltpu.VMEM((count, depth), BF16), pltpu.VMEM((count, depth), BF16), pltpu.VMEM((depth, HEAD_DIM), BF16), pltpu.VMEM((depth, HEAD_DIM), BF16), pltpu.VMEM((depth // SLOT_ROWS, SLOT_ROWS, w_q.shape[1]), BF16), dma((count // 32,)), dma((2,)), dma((depth // SLOT_ROWS,))],
            compiler_params=pltpu.CompilerParams(vmem_limit_bytes=limit),
            name='project',
        )(rows, attn_gain, pos3, freqs, w_q, w_k, w_v)
        attn_rows = pl.pallas_call(
            functools.partial(attend_kernel, cp_size, side),
            out_shape=jax.ShapeDtypeStruct((count, w_q.shape[1]), BF16),
            in_specs=[vmem, vmem, vmem],
            out_specs=vmem,
            scratch_shapes=[pltpu.VMEM((cp_size, 4, piece, HEAD_DIM), BF16), pltpu.VMEM((2, 1, width), F32), pltpu.VMEM((2, 1, width), F32), pltpu.VMEM((2, HEAD_DIM, width), F32), pltpu.VMEM((OWNERS * piece, width), F32), dma((NUM_COPIES,)), dma((NUM_COPIES,))],
            compiler_params=pltpu.CompilerParams(vmem_limit_bytes=limit, collective_id=0, has_side_effects=True),
            name='attend',
        )(kv, q_t, pos3)
        z_rows = pl.pallas_call(
            finish_kernel,
            out_shape=jax.ShapeDtypeStruct((count, depth), BF16),
            in_specs=[hbm, vmem, vmem, hbm, hbm, hbm, hbm],
            out_specs=hbm,
            scratch_shapes=[pltpu.VMEM((count, depth), BF16), pltpu.VMEM((count, depth), BF16), pltpu.VMEM((count, ff), BF16), pltpu.VMEM((2, count, ff // 2), F32), pltpu.VMEM((2, count, SLOT_COLS), BF16), pltpu.VMEM((SLOTS, SLOT_ROWS, SLOT_COLS), BF16), dma(()), dma((SLOTS,)), dma((2,))],
            compiler_params=pltpu.CompilerParams(vmem_limit_bytes=limit),
            name='finish',
        )(rows, attn_rows, mlp_gain, w_o, w_gate, w_up, w_down)
        return z_rows[None], k_rows[:, None, :], v_rows[:, None, :]

    seq_spec = P(('dp', 'cp'))
    return jax.shard_map(device_fn, mesh=mesh, in_specs=(P('dp', 'cp', None), seq_spec, seq_spec, P(), P(), P(), P(), P(), P(), P(), P(), P()), out_specs=(P('dp', 'cp', None), P(('dp', 'cp'), None, None), P(('dp', 'cp'), None, None)), check_vma=False)
```

```python
import functools
import math

import jax
import jax.numpy as jnp
import numpy as np
from jax import lax
from jax.experimental import pallas as pl
from jax.experimental.pallas import tpu as pltpu
from jax.sharding import PartitionSpec as P

HEAD_DIM = 128
ROPE_THETA = 500000.0
ROPE_FACTOR = 8.0
LOW_FREQ = 1.0
HIGH_FREQ = 4.0
ORIG_CTX = 8192.0
NORM_EPS = 1e-5
NEG_BIG = -1e30
SCORE_LOG2 = HEAD_DIM ** -0.5 * math.log2(math.e)
MESH = pl.DeviceIdType.MESH
COLS = 512
SLOTS = 8
SLOT_ROWS = 1024
SLOT_COLS = 2048
OWNERS = 4
LANES = 256
F32 = jnp.float32
BF16 = jnp.bfloat16


def rope_freqs():
    exponent = np.arange(0, HEAD_DIM, 2) / HEAD_DIM
    inv_freq = 1.0 / (ROPE_THETA ** exponent)
    wavelen = 2.0 * np.pi / inv_freq
    smooth = np.clip((ORIG_CTX / wavelen - LOW_FREQ) / (HIGH_FREQ - LOW_FREQ), 0.0, 1.0)
    return ((1.0 - smooth) * inv_freq / ROPE_FACTOR + smooth * inv_freq).astype(np.float32)


def fdot(lhs, rhs):
    return jnp.dot(lhs, rhs, preferred_element_type=F32)


def norm_rows(src_ref, dst_ref, gain_ref, row, count):
    depth = src_ref.shape[1]
    rows = pl.ds(row, count)
    total = jnp.zeros((count, 128), F32)
    for col in range(0, depth, 128):
        part = src_ref[rows, col:col + 128].astype(F32)
        total = total + part * part
    inv_rms = lax.rsqrt(jnp.sum(total, axis=1, keepdims=True) / depth + NORM_EPS)
    for col in range(0, depth, 512):
        part = src_ref[rows, col:col + 512].astype(F32)
        gain = gain_ref[col:col + 512].astype(F32).reshape(1, 512)
        dst_ref[rows, col:col + 512] = (part * inv_rms * gain).astype(BF16)


def project_kernel(x_hbm, gain_ref, pos_ref, freq_ref, wq_hbm, wk_hbm, wv_hbm, qt_ref, kv_ref, kc_ref, vc_ref, x_buf, a_buf, wk_buf, wv_buf, wq_buf, x_sem, wkv_sem, wq_sem):
    count, depth = x_buf.shape
    piece = count // 2
    blocks = x_sem.shape[0]
    rows_blk = count // blocks
    chunks = wq_buf.shape[0]
    chunk_rows = wq_buf.shape[1]

    def x_copy(idx):
        rows = pl.ds(idx * rows_blk, rows_blk)
        return pltpu.make_async_copy(x_hbm.at[rows], x_buf.at[rows], x_sem.at[idx])

    for idx in range(blocks):
        x_copy(idx).start()
    wkv = [pltpu.make_async_copy(wk_hbm, wk_buf, wkv_sem.at[0]), pltpu.make_async_copy(wv_hbm, wv_buf, wkv_sem.at[1])]
    for copy in wkv:
        copy.start()
    wq_copies = [pltpu.make_async_copy(wq_hbm.at[pl.ds(idx * chunk_rows, chunk_rows)], wq_buf.at[idx], wq_sem.at[idx]) for idx in range(chunks)]
    for idx, copy in enumerate(wq_copies):
        copy.start(priority=idx % 2)

    cos_t, sin_t = rope_tables(pos_ref, freq_ref)

    @pl.loop(0, blocks)
    def _(idx):
        x_copy(idx).wait()
        norm_rows(x_buf, a_buf, gain_ref, pl.multiple_of(idx * rows_blk, rows_blk), rows_blk)

    for copy in wkv:
        copy.wait()
    kv_raw = fdot(a_buf[...], jnp.concatenate([wk_buf[...], wv_buf[...]], axis=1))

    def rope(raw):
        return raw * cos_t + pltpu.roll(raw, HEAD_DIM // 2, 1) * sin_t

    k_rot = rope(kv_raw[:, :HEAD_DIM])
    v_raw = kv_raw[:, HEAD_DIM:]
    kc_ref[...] = k_rot.astype(BF16)
    vc_ref[...] = v_raw.astype(BF16)
    for half in range(2):
        rows = slice(half * piece, (half + 1) * piece)
        kv_ref[half] = k_rot[rows].astype(BF16)
        kv_ref[2 + half] = v_raw[rows].T.astype(BF16)

    for copy in wq_copies:
        copy.wait()
    for col in range(wq_hbm.shape[1] // COLS):
        q_raw = fdot(a_buf[...], jnp.concatenate([wq_buf[idx, :, col * COLS:(col + 1) * COLS] for idx in range(chunks)], axis=0))
        for sub in range(COLS // HEAD_DIM):
            head = col * (COLS // HEAD_DIM) + sub
            q_rot = rope(q_raw[:, sub * HEAD_DIM:(sub + 1) * HEAD_DIM])
            for half in range(2):
                qt_ref[half, :, head * piece:(head + 1) * piece] = q_rot[half * piece:(half + 1) * piece].T.astype(BF16)


def rope_tables(pos_ref, freq_ref):
    cos_parts, sin_parts = [], []
    for half in range(2):
        angles = freq_ref[...] * pos_ref[half].astype(F32)
        cos_parts.append(jnp.cos(angles).T)
        sin_parts.append(jnp.sin(angles).T)
    cos_h = jnp.concatenate(cos_parts, axis=0)
    sin_h = jnp.concatenate(sin_parts, axis=0)
    return jnp.concatenate([cos_h, cos_h], axis=1), jnp.concatenate([-sin_h, sin_h], axis=1)


def gather_shards(side, kv_ref, all_ref, send_sem, recv_sem, on_start, on_group):
    me = lax.axis_index('cp')
    core = lax.rem(me, 2)
    chip = me // 2
    chip_x = lax.rem(chip, side)
    chip_y = chip // side

    def owner(first, second, core=core):
        pos_x = lax.rem(chip_x + first * (1 - core) + second * core + 2 * side, side)
        pos_y = lax.rem(chip_y + first * core + second * (1 - core) + 2 * side, side)
        return (pos_y * side + pos_x) * 2 + core

    def other(first, second):
        return owner(first, second, 1 - core)

    sibling = me + 1 - 2 * core
    targets = {'a+': owner(1, 0), 'a-': owner(-1, 0), 'b+': owner(0, 1), 'b-': owner(0, -1), 's': sibling}
    barrier = pltpu.get_barrier_semaphore()
    for target in targets.values():
        pl.semaphore_signal(barrier, inc=1, device_id={'cp': target}, device_id_type=MESH)
    pl.semaphore_wait(barrier, len(targets))

    copies = []

    def send(shard, where, half=None):
        num = len(copies)
        dst = all_ref.at[shard]
        src = kv_ref if num < 5 else dst
        if half is not None:
            dst = dst.at[pl.ds(2 * half, 2)]
            src = dst
        copy = pltpu.make_async_remote_copy(src_ref=src, dst_ref=dst, send_sem=send_sem.at[num], recv_sem=recv_sem.at[num], device_id={'cp': targets[where]}, device_id_type=MESH)
        copy.start()
        copies.append(copy)
        return copy

    from_sibling = []

    def spread(shard):
        plus = send(shard, 'b+')
        minus = send(shard, 'b-')
        from_sibling.append(send(shard, 's'))
        return plus, minus

    own_right = send(me, 'a+')
    own_left = send(me, 'a-')
    row_own = spread(me)
    all_ref[me] = kv_ref[...]
    on_start()
    own_right.wait_recv()
    shard = owner(-1, 0)
    far_k = send(shard, 'a+', 0)
    row_left = spread(shard)
    own_left.wait_recv()
    shard = owner(1, 0)
    far_v = send(shard, 'a-', 1)
    row_right = spread(shard)

    def relay(first, row):
        row[0].wait_recv()
        shard = owner(first, -1)
        half_k = send(shard, 'b+', 0)
        from_sibling.append(send(shard, 's'))
        row[1].wait_recv()
        shard = owner(first, 1)
        half_v = send(shard, 'b-', 1)
        from_sibling.append(send(shard, 's'))
        return half_k, half_v

    def close(first, halves):
        halves[0].wait_recv()
        halves[1].wait_recv()
        from_sibling.append(send(owner(first, 2), 's'))

    def arrived(*nums):
        for num in nums:
            from_sibling[num].wait_recv()

    arrived(0)
    on_group(me, sibling, owner(-1, 0), owner(1, 0))
    far_own = relay(0, row_own)
    far_k.wait_recv()
    far_v.wait_recv()
    row_far = spread(owner(2, 0))
    arrived(1, 2)
    on_group(owner(0, -1), owner(0, 1), other(-1, 0), other(1, 0))
    far_left = relay(-1, row_left)
    far_right = relay(1, row_right)
    arrived(3, 4)
    on_group(owner(2, 0), owner(-1, -1), other(0, -1), other(0, 1))
    close(0, far_own)
    far_far = relay(2, row_far)
    arrived(5)
    on_group(owner(-1, 1), owner(1, -1), owner(1, 1), other(2, 0))
    close(-1, far_left)
    close(1, far_right)
    arrived(6, 7)
    on_group(owner(0, 2), owner(2, -1), other(-1, -1), other(-1, 1))
    close(2, far_far)
    arrived(8, 9)
    on_group(owner(2, 1), owner(-1, 2), other(1, -1), other(1, 1))
    arrived(10, 11)
    on_group(owner(1, 2), owner(2, 2), other(0, 2), other(2, -1))
    arrived(12, 13, 14, 15)
    on_group(other(2, 1), other(-1, 2), other(1, 2), other(2, 2))
    for copy in copies:
        copy.wait_send()


NUM_COPIES = 36


def attend_kernel(cp_size, side, kv_ref, qt_ref, pos_ref, out_ref, all_ref, max_ref, sum_ref, acc_ref, score_ref, send_sem, recv_sem):
    me = lax.axis_index('cp')
    piece = kv_ref.shape[1]
    width = qt_ref.shape[2]
    tiles = width // LANES
    bases = (me * piece, (2 * cp_size - 1 - me) * piece)
    lane_tok = lax.broadcasted_iota(jnp.int32, (1, piece), 1)

    def starts(half):
        first = bases[half] + lane_tok - pos_ref[half]
        return jnp.concatenate([first] * (LANES // piece), axis=1)

    first_key = (starts(0), starts(1))
    tok = jnp.concatenate([lane_tok] * (LANES // piece), axis=1)
    key_row = lax.broadcasted_iota(jnp.int32, (piece, LANES), 0)

    def diagonal():
        for half in range(2):
            visible = (key_row <= tok) & (key_row + bases[half] >= first_key[half])
            for tile in range(tiles):
                cols = slice(tile * LANES, (tile + 1) * LANES)
                scores = fdot(kv_ref[half], qt_ref[half, :, cols])
                scores = jnp.where(visible, scores, NEG_BIG)
                top = jnp.max(scores, axis=0, keepdims=True)
                prob = jnp.exp2((scores - top) * SCORE_LOG2)
                max_ref[half, :, cols] = top
                sum_ref[half, :, cols] = jnp.sum(prob, axis=0, keepdims=True)
                acc_ref[half, :, cols] = fdot(kv_ref[2 + half], prob.astype(BF16))

    def block(half, part, owners, key_base):
        keys = jnp.concatenate([all_ref[own, part] for own in owners], axis=0)
        vals = jnp.concatenate([all_ref[own, 2 + part] for own in owners], axis=1)
        hidden = [key_row < first_key[half] - base for base in key_base]
        tops, scales = [], []
        for tile in range(tiles):
            cols = slice(tile * LANES, (tile + 1) * LANES)
            raw = fdot(keys, qt_ref[half, :, cols])
            peak = None
            for sub in range(OWNERS):
                rows = slice(sub * piece, (sub + 1) * piece)
                score = jnp.where(hidden[sub], NEG_BIG, raw[rows])
                score_ref[rows, cols] = score
                best = jnp.max(score, axis=0, keepdims=True)
                peak = best if peak is None else jnp.maximum(peak, best)
            old_top = max_ref[half, :, cols]
            top = jnp.maximum(old_top, peak)
            max_ref[half, :, cols] = top
            tops.append(top)
            scales.append(jnp.exp2((old_top - top) * SCORE_LOG2))
        for tile in range(tiles):
            cols = slice(tile * LANES, (tile + 1) * LANES)
            prob = jnp.exp2((score_ref[:, cols] - tops[tile]) * SCORE_LOG2)
            sum_ref[half, :, cols] = sum_ref[half, :, cols] * scales[tile] + jnp.sum(prob, axis=0, keepdims=True)
            acc_ref[half, :, cols] = acc_ref[half, :, cols] * scales[tile] + fdot(vals, prob.astype(BF16))

    def low_group(*owners):
        block(1, 0, owners, [own * piece for own in owners])

    gather_shards(side, kv_ref, all_ref, send_sem, recv_sem, diagonal, low_group)

    @pl.loop(0, (me + OWNERS - 1) // OWNERS)
    def _(idx):
        owners = [idx * OWNERS + sub for sub in range(OWNERS)]
        block(0, 0, owners, [jnp.where(own < me, own * piece, -2 * piece) for own in owners])

    @pl.loop((me + 1) // OWNERS, cp_size // OWNERS)
    def _(idx):
        owners = [idx * OWNERS + sub for sub in range(OWNERS)]
        block(1, 1, owners, [jnp.where(own > me, (2 * cp_size - 1 - own) * piece, -2 * piece) for own in owners])

    for half in range(2):
        for head in range(width // piece):
            cols = slice(head * piece, (head + 1) * piece)
            done = acc_ref[half, :, cols] / sum_ref[half, :, cols]
            out_ref[half * piece:(half + 1) * piece, head * HEAD_DIM:(head + 1) * HEAD_DIM] = done.T.astype(BF16)


def finish_kernel(x_hbm, attn_ref, gain_ref, wo_hbm, wg_hbm, wu_hbm, wd_hbm, z_hbm, h_buf, b_buf, m_buf, acc_ref, z_buf, slots, x_sem, slot_sem, z_sem):
    count, depth = h_buf.shape
    ff = wg_hbm.shape[1]
    ff_half = ff // 2
    group = 4
    n_wo = depth // SLOT_COLS
    k_steps = depth // (SLOT_ROWS * group)
    n_ff = 4 * k_steps
    dn_rows = [min(SLOT_ROWS, ff - row) for row in range(0, ff, SLOT_ROWS)]
    n_dn = depth // SLOT_COLS
    ff_from = n_wo
    dn_from = ff_from + n_ff * group
    total = dn_from + n_dn * len(dn_rows)

    def cols_of(idx, size):
        return pl.ds(pl.multiple_of(idx * size, size), size)

    def halves(src, dst, rows, sem):
        for part in range(2):
            sel = pl.ds(part * rows // 2, rows // 2)
            pltpu.make_async_copy(src.at[sel], dst.at[sel], sem).start(priority=part)

    def issue(num):
        slot = lax.rem(num, SLOTS)
        sem = slot_sem.at[slot]
        dst = slots.at[slot]

        @pl.when(num < ff_from)
        def _():
            halves(wo_hbm.at[:, cols_of(num, SLOT_COLS)], dst, SLOT_ROWS, sem)

        rel = num - ff_from
        step = rel // group
        half = step // (2 * k_steps)
        kind = lax.rem(step // k_steps, 2)
        row = cols_of(lax.rem(step, k_steps) * group + lax.rem(rel, group), SLOT_ROWS)
        in_ff = (num >= ff_from) & (num < dn_from)

        @pl.when(in_ff & (kind == 0))
        def _():
            halves(wg_hbm.at[row, cols_of(half, ff_half)], dst.at[:, pl.ds(0, ff_half)], SLOT_ROWS, sem)

        @pl.when(in_ff & (kind == 1))
        def _():
            halves(wu_hbm.at[row, cols_of(half, ff_half)], dst.at[:, pl.ds(0, ff_half)], SLOT_ROWS, sem)

        rel = num - dn_from
        for idx, rows in enumerate(dn_rows):
            @pl.when((num >= dn_from) & (num < total) & (lax.rem(rel, len(dn_rows)) == idx))
            def _():
                src = wd_hbm.at[pl.ds(idx * SLOT_ROWS, rows), cols_of(rel // len(dn_rows), SLOT_COLS)]
                halves(src, dst.at[pl.ds(0, rows)], rows, sem)

    def take(num, rows, cols):
        slot = lax.rem(num, SLOTS)
        part = slots.at[slot, pl.ds(0, rows), pl.ds(0, cols)]
        pltpu.make_async_copy(part, part, slot_sem.at[slot]).wait()
        return slots.at[slot]

    x_copy = pltpu.make_async_copy(x_hbm, h_buf, x_sem)
    x_copy.start()
    for num in range(SLOTS):
        issue(jnp.int32(num))
    x_copy.wait()

    @pl.loop(0, n_wo)
    def _(num):
        slot = take(num, SLOT_ROWS, SLOT_COLS)
        for sub in range(0, SLOT_COLS, COLS):
            cols = pl.ds(pl.multiple_of(num * SLOT_COLS + sub, COLS), COLS)
            out = fdot(attn_ref[...], slot[:, sub:sub + COLS])
            h_buf[:, cols] = (h_buf[:, cols].astype(F32) + out).astype(BF16)
        issue(num + SLOTS)

    @pl.loop(0, count // 32)
    def _(idx):
        norm_rows(h_buf, b_buf, gain_ref, pl.multiple_of(idx * 32, 32), 32)

    @pl.loop(0, n_ff)
    def _(step):
        num = ff_from + step * group
        half = step // (2 * k_steps)
        kind = lax.rem(step // k_steps, 2)
        k_idx = lax.rem(step, k_steps)
        parts = [take(num + sub, SLOT_ROWS, ff_half) for sub in range(group)]
        lhs = b_buf[:, cols_of(k_idx, SLOT_ROWS * group)]
        for col in range(0, ff_half, COLS):
            size = min(COLS, ff_half - col)
            cols = slice(col, col + size)
            out = fdot(lhs, jnp.concatenate([part[:, cols] for part in parts], axis=0))
            acc_ref[kind, :, cols] = jnp.where(k_idx == 0, 0.0, acc_ref[kind, :, cols]) + out
        for sub in range(group):
            issue(num + sub + SLOTS)

        @pl.when((kind == 1) & (k_idx == k_steps - 1))
        def _():
            for col in range(0, ff_half, 256):
                gate = acc_ref[0, :, col:col + 256]
                dst = pl.ds(pl.multiple_of(half * ff_half + col, 256), 256)
                m_buf[:, dst] = (gate * jax.nn.sigmoid(gate) * acc_ref[1, :, col:col + 256]).astype(BF16)

    def z_copy(blk):
        slot = lax.rem(blk, 2)
        return pltpu.make_async_copy(z_buf.at[slot], z_hbm.at[:, cols_of(blk, SLOT_COLS)], z_sem.at[slot])

    @pl.loop(0, n_dn)
    def _(blk):
        num = dn_from + blk * len(dn_rows)
        parts = [take(num + idx, rows, SLOT_COLS) for idx, rows in enumerate(dn_rows)]

        @pl.when(blk >= 2)
        def _():
            z_copy(blk - 2).wait()

        for sub in range(0, SLOT_COLS, COLS):
            cols = pl.ds(pl.multiple_of(blk * SLOT_COLS + sub, COLS), COLS)
            out = fdot(m_buf[...], jnp.concatenate([part[:rows, sub:sub + COLS] for part, rows in zip(parts, dn_rows)], axis=0))
            z_buf[lax.rem(blk, 2), :, sub:sub + COLS] = (h_buf[:, cols].astype(F32) + out).astype(BF16)
        z_copy(blk).start()
        for idx in range(len(dn_rows)):
            issue(num + idx + SLOTS)

    for blk in range(max(0, n_dn - 2), n_dn):
        z_copy(blk).wait()


def solution(mesh):
    cp_size = mesh.shape['cp']
    side = math.isqrt(cp_size // 2)
    vmem = pl.BlockSpec(memory_space=pltpu.VMEM)
    hbm = pl.BlockSpec(memory_space=pl.ANY)
    dma = pltpu.SemaphoreType.DMA
    limit = 60 * 1024 * 1024

    def device_fn(x_loc, seg_loc, pos_loc, attn_gain, w_q, w_k, w_v, w_o, mlp_gain, w_gate, w_up, w_down):
        rows = x_loc[0]
        count, depth = rows.shape
        piece = count // 2
        width = w_q.shape[1] // HEAD_DIM * piece
        ff = w_gate.shape[1]
        pos3 = pos_loc.reshape(2, 1, piece)
        freqs = jnp.asarray(rope_freqs()).reshape(HEAD_DIM // 2, 1)
        q_t, kv, k_rows, v_rows = pl.pallas_call(
            project_kernel,
            out_shape=(jax.ShapeDtypeStruct((2, HEAD_DIM, width), BF16), jax.ShapeDtypeStruct((4, piece, HEAD_DIM), BF16), jax.ShapeDtypeStruct((count, HEAD_DIM), BF16), jax.ShapeDtypeStruct((count, HEAD_DIM), BF16)),
            in_specs=[hbm, vmem, vmem, vmem, hbm, hbm, hbm],
            out_specs=(vmem, vmem, vmem, vmem),
            scratch_shapes=[pltpu.VMEM((count, depth), BF16), pltpu.VMEM((count, depth), BF16), pltpu.VMEM((depth, HEAD_DIM), BF16), pltpu.VMEM((depth, HEAD_DIM), BF16), pltpu.VMEM((depth // SLOT_ROWS, SLOT_ROWS, w_q.shape[1]), BF16), dma((count // 32,)), dma((2,)), dma((depth // SLOT_ROWS,))],
            compiler_params=pltpu.CompilerParams(vmem_limit_bytes=limit),
            name='project',
        )(rows, attn_gain, pos3, freqs, w_q, w_k, w_v)
        attn_rows = pl.pallas_call(
            functools.partial(attend_kernel, cp_size, side),
            out_shape=jax.ShapeDtypeStruct((count, w_q.shape[1]), BF16),
            in_specs=[vmem, vmem, vmem],
            out_specs=vmem,
            scratch_shapes=[pltpu.VMEM((cp_size, 4, piece, HEAD_DIM), BF16), pltpu.VMEM((2, 1, width), F32), pltpu.VMEM((2, 1, width), F32), pltpu.VMEM((2, HEAD_DIM, width), F32), pltpu.VMEM((OWNERS * piece, width), F32), dma((NUM_COPIES,)), dma((NUM_COPIES,))],
            compiler_params=pltpu.CompilerParams(vmem_limit_bytes=limit, collective_id=0, has_side_effects=True),
            name='attend',
        )(kv, q_t, pos3)
        z_rows = pl.pallas_call(
            finish_kernel,
            out_shape=jax.ShapeDtypeStruct((count, depth), BF16),
            in_specs=[hbm, vmem, vmem, hbm, hbm, hbm, hbm],
            out_specs=hbm,
            scratch_shapes=[pltpu.VMEM((count, depth), BF16), pltpu.VMEM((count, depth), BF16), pltpu.VMEM((count, ff), BF16), pltpu.VMEM((2, count, ff // 2), F32), pltpu.VMEM((2, count, SLOT_COLS), BF16), pltpu.VMEM((SLOTS, SLOT_ROWS, SLOT_COLS), BF16), dma(()), dma((SLOTS,)), dma((2,))],
            compiler_params=pltpu.CompilerParams(vmem_limit_bytes=limit),
            name='finish',
        )(rows, attn_rows, mlp_gain, w_o, w_gate, w_up, w_down)
        return z_rows[None], k_rows[:, None, :], v_rows[:, None, :]

    seq_spec = P(('dp', 'cp'))
    return jax.shard_map(device_fn, mesh=mesh, in_specs=(P('dp', 'cp', None), seq_spec, seq_spec, P(), P(), P(), P(), P(), P(), P(), P(), P()), out_specs=(P('dp', 'cp', None), P(('dp', 'cp'), None, None), P(('dp', 'cp'), None, None)), check_vma=False)
```

```python
import functools
import math

import jax
import jax.numpy as jnp
import numpy as np
from jax import lax
from jax.experimental import pallas as pl
from jax.experimental.pallas import tpu as pltpu
from jax.sharding import PartitionSpec as P

HEAD_DIM = 128
ROPE_THETA = 500000.0
ROPE_FACTOR = 8.0
LOW_FREQ = 1.0
HIGH_FREQ = 4.0
ORIG_CTX = 8192.0
NORM_EPS = 1e-5
NEG_BIG = -1e30
SCORE_LOG2 = HEAD_DIM ** -0.5 * math.log2(math.e)
MESH = pl.DeviceIdType.MESH
COLS = 512
SLOTS = 8
SLOT_ROWS = 1024
SLOT_COLS = 2048
OWNERS = 4
LANES = 512
F32 = jnp.float32
BF16 = jnp.bfloat16


def rope_freqs():
    exponent = np.arange(0, HEAD_DIM, 2) / HEAD_DIM
    inv_freq = 1.0 / (ROPE_THETA ** exponent)
    wavelen = 2.0 * np.pi / inv_freq
    smooth = np.clip((ORIG_CTX / wavelen - LOW_FREQ) / (HIGH_FREQ - LOW_FREQ), 0.0, 1.0)
    return ((1.0 - smooth) * inv_freq / ROPE_FACTOR + smooth * inv_freq).astype(np.float32)


def fdot(lhs, rhs):
    return jnp.dot(lhs, rhs, preferred_element_type=F32)


def norm_rows(src_ref, dst_ref, gain_ref, row, count):
    depth = src_ref.shape[1]
    rows = pl.ds(row, count)
    total = jnp.zeros((count, 128), F32)
    for col in range(0, depth, 128):
        part = src_ref[rows, col:col + 128].astype(F32)
        total = total + part * part
    inv_rms = lax.rsqrt(jnp.sum(total, axis=1, keepdims=True) / depth + NORM_EPS)
    for col in range(0, depth, 512):
        part = src_ref[rows, col:col + 512].astype(F32)
        gain = gain_ref[col:col + 512].astype(F32).reshape(1, 512)
        dst_ref[rows, col:col + 512] = (part * inv_rms * gain).astype(BF16)


def project_kernel(x_hbm, gain_ref, pos_ref, freq_ref, wk_hbm, wv_hbm, a_hbm, cos_ref, sin_ref, kv_ref, kc_ref, vc_ref, x_buf, a_buf, wk_buf, wv_buf, x_sem, wkv_sem, a_sem):
    count = x_buf.shape[0]
    piece = count // 2
    blocks = x_sem.shape[0]
    rows_blk = count // blocks

    def x_copy(idx):
        rows = pl.ds(idx * rows_blk, rows_blk)
        return pltpu.make_async_copy(x_hbm.at[rows], x_buf.at[rows], x_sem.at[idx])

    def a_copy(idx):
        rows = pl.ds(idx * rows_blk, rows_blk)
        return pltpu.make_async_copy(a_buf.at[rows], a_hbm.at[rows], a_sem.at[idx])

    for idx in range(blocks):
        x_copy(idx).start()
    wkv = [pltpu.make_async_copy(wk_hbm, wk_buf, wkv_sem.at[0]), pltpu.make_async_copy(wv_hbm, wv_buf, wkv_sem.at[1])]
    for copy in wkv:
        copy.start(priority=1)
    for half in range(2):
        rows = slice(half * piece, (half + 1) * piece)
        angles = freq_ref[...] * pos_ref[half].astype(F32)
        cos_h = jnp.cos(angles).T
        sin_h = jnp.sin(angles).T
        cos_ref[rows] = jnp.concatenate([cos_h, cos_h], axis=1)
        sin_ref[rows] = jnp.concatenate([-sin_h, sin_h], axis=1)

    @pl.loop(0, blocks)
    def _(idx):
        x_copy(idx).wait()
        norm_rows(x_buf, a_buf, gain_ref, pl.multiple_of(idx * rows_blk, rows_blk), rows_blk)
        a_copy(idx).start()

    for copy in wkv:
        copy.wait()
    kv_raw = fdot(a_buf[...], jnp.concatenate([wk_buf[...], wv_buf[...]], axis=1))
    k_rot = rope(kv_raw[:, :HEAD_DIM], cos_ref[...], sin_ref[...])
    v_raw = kv_raw[:, HEAD_DIM:]
    kc_ref[...] = k_rot.astype(BF16)
    vc_ref[...] = v_raw.astype(BF16)
    for half in range(2):
        rows = slice(half * piece, (half + 1) * piece)
        kv_ref[half] = k_rot[rows].astype(BF16)
        kv_ref[2 + half] = v_raw[rows].T.astype(BF16)
    for idx in range(blocks):
        a_copy(idx).wait()


def rope(raw, cos_t, sin_t):
    half = HEAD_DIM // 2
    return raw * cos_t + jnp.concatenate([raw[:, half:], raw[:, :half]], axis=1) * sin_t


def torus_place(side):
    me = lax.axis_index('cp')
    core = lax.rem(me, 2)
    chip = me // 2
    chip_x = lax.rem(chip, side)
    chip_y = chip // side

    def owner(first, second, core=core):
        pos_x = lax.rem(chip_x + first * (1 - core) + second * core + 2 * side, side)
        pos_y = lax.rem(chip_y + first * core + second * (1 - core) + 2 * side, side)
        return (pos_y * side + pos_x) * 2 + core

    def other(first, second):
        return owner(first, second, 1 - core)

    return me, owner, other


def gather_shards(place, kv_ref, all_ref, send_sem, recv_sem, on_start, on_group):
    me, owner, other = place
    sibling = other(0, 0)
    targets = {'a+': owner(1, 0), 'a-': owner(-1, 0), 'b+': owner(0, 1), 'b-': owner(0, -1), 's': sibling}
    barrier = pltpu.get_barrier_semaphore()
    for target in targets.values():
        pl.semaphore_signal(barrier, inc=1, device_id={'cp': target}, device_id_type=MESH)
    pl.semaphore_wait(barrier, len(targets))

    copies = []

    def send(shard, where, half=None):
        num = len(copies)
        dst = all_ref.at[shard]
        src = kv_ref if num < 5 else dst
        if half is not None:
            dst = dst.at[pl.ds(2 * half, 2)]
            src = dst
        copy = pltpu.make_async_remote_copy(src_ref=src, dst_ref=dst, send_sem=send_sem.at[num], recv_sem=recv_sem.at[num], device_id={'cp': targets[where]}, device_id_type=MESH)
        copy.start()
        copies.append(copy)
        return copy

    from_sibling = []

    def spread(shard):
        plus = send(shard, 'b+')
        minus = send(shard, 'b-')
        from_sibling.append(send(shard, 's'))
        return plus, minus

    def relay(first, row):
        row[0].wait_recv()
        shard = owner(first, -1)
        half_k = send(shard, 'b+', 0)
        from_sibling.append(send(shard, 's'))
        row[1].wait_recv()
        shard = owner(first, 1)
        half_v = send(shard, 'b-', 1)
        from_sibling.append(send(shard, 's'))
        return half_k, half_v

    def close(first, halves):
        halves[0].wait_recv()
        halves[1].wait_recv()
        from_sibling.append(send(owner(first, 2), 's'))

    def arrived(*nums):
        for num in nums:
            from_sibling[num].wait_recv()

    own_right = send(me, 'a+')
    own_left = send(me, 'a-')
    row_own = spread(me)
    all_ref[me] = kv_ref[...]
    on_start()
    own_right.wait_recv()
    shard = owner(-1, 0)
    far_k = send(shard, 'a+', 0)
    row_left = spread(shard)
    own_left.wait_recv()
    shard = owner(1, 0)
    far_v = send(shard, 'a-', 1)
    row_right = spread(shard)
    far_own = relay(0, row_own)
    arrived(0)
    on_group(me, sibling, owner(-1, 0), owner(1, 0))
    far_k.wait_recv()
    far_v.wait_recv()
    row_far = spread(owner(2, 0))
    arrived(1, 2)
    on_group(owner(0, -1), owner(0, 1), other(-1, 0), other(1, 0))
    far_left = relay(-1, row_left)
    far_right = relay(1, row_right)
    arrived(3, 4)
    on_group(owner(2, 0), owner(-1, -1), other(0, -1), other(0, 1))
    close(0, far_own)
    far_far = relay(2, row_far)
    arrived(5)
    on_group(owner(-1, 1), owner(1, -1), owner(1, 1), other(2, 0))
    close(-1, far_left)
    close(1, far_right)
    arrived(6, 7)
    on_group(owner(0, 2), owner(2, -1), other(-1, -1), other(-1, 1))
    close(2, far_far)
    arrived(8, 9)
    on_group(owner(2, 1), owner(-1, 2), other(1, -1), other(1, 1))
    arrived(10, 11)
    on_group(owner(1, 2), owner(2, 2), other(0, 2), other(2, -1))
    arrived(12, 13, 14, 15)
    on_group(other(2, 1), other(-1, 2), other(1, 2), other(2, 2))
    for copy in copies:
        copy.wait_send()


NUM_COPIES = 36


def attend_kernel(cp_size, side, kv_ref, pos_ref, cos_ref, sin_ref, a_hbm, wq_hbm, out_ref, a_buf, wq_buf, qt_ref, all_ref, max_ref, sum_ref, acc_ref, score_ref, a_sem, wq_sem, send_sem, recv_sem):
    place = torus_place(side)
    me = place[0]
    count = a_buf.shape[0]
    piece = count // 2
    width = qt_ref.shape[2]
    tiles = width // LANES
    chunks, chunk_rows = wq_buf.shape[:2]
    loads = [pltpu.make_async_copy(a_hbm, a_buf, a_sem)]
    loads += [pltpu.make_async_copy(wq_hbm.at[pl.ds(idx * chunk_rows, chunk_rows)], wq_buf.at[idx], wq_sem.at[idx]) for idx in range(chunks)]
    for copy in loads:
        copy.start()

    bases = (me * piece, (2 * cp_size - 1 - me) * piece)
    lane_tok = lax.broadcasted_iota(jnp.int32, (1, piece), 1)

    def starts(half):
        first = bases[half] + lane_tok - pos_ref[half]
        return jnp.concatenate([first] * (LANES // piece), axis=1)

    first_key = (starts(0), starts(1))
    tok = jnp.concatenate([lane_tok] * (LANES // piece), axis=1)
    key_row = lax.broadcasted_iota(jnp.int32, (piece, LANES), 0)

    def queries_and_diagonal():
        for copy in loads:
            copy.wait()
        for col in range(wq_buf.shape[2] // COLS):
            q_raw = fdot(a_buf[...], jnp.concatenate([wq_buf[idx, :, col * COLS:(col + 1) * COLS] for idx in range(chunks)], axis=0))
            for sub in range(COLS // HEAD_DIM):
                head = col * (COLS // HEAD_DIM) + sub
                q_rot = rope(q_raw[:, sub * HEAD_DIM:(sub + 1) * HEAD_DIM], cos_ref[...], sin_ref[...])
                for half in range(2):
                    qt_ref[half, :, head * piece:(head + 1) * piece] = q_rot[half * piece:(half + 1) * piece].T.astype(BF16)
        for half in range(2):
            visible = (key_row <= tok) & (key_row + bases[half] >= first_key[half])

            @pl.loop(0, tiles)
            def _(tile):
                cols = pl.ds(pl.multiple_of(tile * LANES, LANES), LANES)
                scores = fdot(kv_ref[half], qt_ref[half, :, cols])
                scores = jnp.where(visible, scores, NEG_BIG)
                top = jnp.max(scores, axis=0, keepdims=True)
                prob = jnp.exp2((scores - top) * SCORE_LOG2)
                max_ref[half, :, cols] = top
                sum_ref[half, :, cols] = jnp.sum(prob, axis=0, keepdims=True)
                acc_ref[half, :, cols] = fdot(kv_ref[2 + half], prob.astype(BF16))

    def low_tile(owners, cols):
        keys = jnp.concatenate([all_ref[own, 0] for own in owners], axis=0)
        vals = jnp.concatenate([all_ref[own, 2] for own in owners], axis=1)
        raw = fdot(keys, qt_ref[1, :, cols])
        peak = None
        for sub, own in enumerate(owners):
            rows = slice(sub * piece, (sub + 1) * piece)
            score = jnp.where(key_row < first_key[1] - own * piece, NEG_BIG, raw[rows])
            score_ref[rows] = score
            best = jnp.max(score, axis=0, keepdims=True)
            peak = best if peak is None else jnp.maximum(peak, best)
        old_top = max_ref[1, :, cols]
        top = jnp.maximum(old_top, peak)
        scale = jnp.exp2((old_top - top) * SCORE_LOG2)
        prob = jnp.exp2((score_ref[...] - top) * SCORE_LOG2)
        max_ref[1, :, cols] = top
        sum_ref[1, :, cols] = sum_ref[1, :, cols] * scale + jnp.sum(prob, axis=0, keepdims=True)
        acc_ref[1, :, cols] = acc_ref[1, :, cols] * scale + fdot(vals, prob.astype(BF16))

    def side_tile(own, cols):
        half = (own - me + cp_size) // cp_size
        base = (own + half * (2 * cp_size - 1 - 2 * own)) * piece
        hidden = key_row < jnp.where(half == 0, first_key[0], first_key[1]) - base
        score = jnp.where(hidden, NEG_BIG, fdot(all_ref[own, half], qt_ref[half, :, cols]))
        old_top = max_ref[half, :, cols]
        top = jnp.maximum(old_top, jnp.max(score, axis=0, keepdims=True))
        prob = jnp.exp2((score - top) * SCORE_LOG2)
        scale = jnp.exp2((old_top - top) * SCORE_LOG2)
        max_ref[half, :, cols] = top
        sum_ref[half, :, cols] = sum_ref[half, :, cols] * scale + jnp.sum(prob, axis=0, keepdims=True)
        acc_ref[half, :, cols] = acc_ref[half, :, cols] * scale + fdot(all_ref[own, 2 + half], prob.astype(BF16))

    def on_group(*owners):
        @pl.loop(0, tiles)
        def _(tile):
            cols = pl.ds(pl.multiple_of(tile * LANES, LANES), LANES)
            low_tile(owners, cols)
            for own in owners:
                if own is not me:
                    side_tile(own, cols)

    gather_shards(place, kv_ref, all_ref, send_sem, recv_sem, queries_and_diagonal, on_group)

    for half in range(2):
        for head in range(width // piece):
            cols = slice(head * piece, (head + 1) * piece)
            done = acc_ref[half, :, cols] / sum_ref[half, :, cols]
            out_ref[half * piece:(half + 1) * piece, head * HEAD_DIM:(head + 1) * HEAD_DIM] = done.T.astype(BF16)


def finish_kernel(x_hbm, attn_ref, gain_ref, wo_hbm, wg_hbm, wu_hbm, wd_hbm, z_hbm, h_buf, b_buf, m_buf, acc_ref, z_buf, slots, x_sem, slot_sem, z_sem):
    count, depth = h_buf.shape
    ff = wg_hbm.shape[1]
    ff_half = ff // 2
    group = 4
    n_wo = depth // SLOT_COLS
    k_steps = depth // (SLOT_ROWS * group)
    n_ff = 4 * k_steps
    dn_rows = [min(SLOT_ROWS, ff - row) for row in range(0, ff, SLOT_ROWS)]
    n_dn = depth // SLOT_COLS
    ff_from = n_wo
    dn_from = ff_from + n_ff * group
    total = dn_from + n_dn * len(dn_rows)

    def cols_of(idx, size):
        return pl.ds(pl.multiple_of(idx * size, size), size)

    def halves(src, dst, rows, sem):
        for part in range(2):
            sel = pl.ds(part * rows // 2, rows // 2)
            pltpu.make_async_copy(src.at[sel], dst.at[sel], sem).start(priority=part)

    def issue(num):
        slot = lax.rem(num, SLOTS)
        sem = slot_sem.at[slot]
        dst = slots.at[slot]

        @pl.when(num < ff_from)
        def _():
            halves(wo_hbm.at[:, cols_of(num, SLOT_COLS)], dst, SLOT_ROWS, sem)

        rel = num - ff_from
        step = rel // group
        half = step // (2 * k_steps)
        kind = lax.rem(step // k_steps, 2)
        row = cols_of(lax.rem(step, k_steps) * group + lax.rem(rel, group), SLOT_ROWS)
        in_ff = (num >= ff_from) & (num < dn_from)

        @pl.when(in_ff & (kind == 0))
        def _():
            halves(wg_hbm.at[row, cols_of(half, ff_half)], dst.at[:, pl.ds(0, ff_half)], SLOT_ROWS, sem)

        @pl.when(in_ff & (kind == 1))
        def _():
            halves(wu_hbm.at[row, cols_of(half, ff_half)], dst.at[:, pl.ds(0, ff_half)], SLOT_ROWS, sem)

        rel = num - dn_from
        for idx, rows in enumerate(dn_rows):
            @pl.when((num >= dn_from) & (num < total) & (lax.rem(rel, len(dn_rows)) == idx))
            def _():
                src = wd_hbm.at[pl.ds(idx * SLOT_ROWS, rows), cols_of(rel // len(dn_rows), SLOT_COLS)]
                halves(src, dst.at[pl.ds(0, rows)], rows, sem)

    def take(num, rows, cols):
        slot = lax.rem(num, SLOTS)
        part = slots.at[slot, pl.ds(0, rows), pl.ds(0, cols)]
        pltpu.make_async_copy(part, part, slot_sem.at[slot]).wait()
        return slots.at[slot]

    x_copy = pltpu.make_async_copy(x_hbm, h_buf, x_sem)
    x_copy.start()
    for num in range(SLOTS):
        issue(jnp.int32(num))
    x_copy.wait()

    @pl.loop(0, n_wo)
    def _(num):
        slot = take(num, SLOT_ROWS, SLOT_COLS)
        for sub in range(0, SLOT_COLS, COLS):
            cols = pl.ds(pl.multiple_of(num * SLOT_COLS + sub, COLS), COLS)
            out = fdot(attn_ref[...], slot[:, sub:sub + COLS])
            h_buf[:, cols] = (h_buf[:, cols].astype(F32) + out).astype(BF16)
        issue(num + SLOTS)

    @pl.loop(0, count // 32)
    def _(idx):
        norm_rows(h_buf, b_buf, gain_ref, pl.multiple_of(idx * 32, 32), 32)

    @pl.loop(0, n_ff)
    def _(step):
        num = ff_from + step * group
        half = step // (2 * k_steps)
        kind = lax.rem(step // k_steps, 2)
        k_idx = lax.rem(step, k_steps)
        parts = [take(num + sub, SLOT_ROWS, ff_half) for sub in range(group)]
        lhs = b_buf[:, cols_of(k_idx, SLOT_ROWS * group)]
        for col in range(0, ff_half, COLS):
            size = min(COLS, ff_half - col)
            cols = slice(col, col + size)
            out = fdot(lhs, jnp.concatenate([part[:, cols] for part in parts], axis=0))
            acc_ref[kind, :, cols] = jnp.where(k_idx == 0, 0.0, acc_ref[kind, :, cols]) + out
        for sub in range(group):
            issue(num + sub + SLOTS)

        @pl.when((kind == 1) & (k_idx == k_steps - 1))
        def _():
            for col in range(0, ff_half, 256):
                gate = acc_ref[0, :, col:col + 256]
                dst = pl.ds(pl.multiple_of(half * ff_half + col, 256), 256)
                m_buf[:, dst] = (gate * jax.nn.sigmoid(gate) * acc_ref[1, :, col:col + 256]).astype(BF16)

    def z_copy(blk):
        slot = lax.rem(blk, 2)
        return pltpu.make_async_copy(z_buf.at[slot], z_hbm.at[:, cols_of(blk, SLOT_COLS)], z_sem.at[slot])

    @pl.loop(0, n_dn)
    def _(blk):
        num = dn_from + blk * len(dn_rows)
        parts = [take(num + idx, rows, SLOT_COLS) for idx, rows in enumerate(dn_rows)]

        @pl.when(blk >= 2)
        def _():
            z_copy(blk - 2).wait()

        for sub in range(0, SLOT_COLS, COLS):
            cols = pl.ds(pl.multiple_of(blk * SLOT_COLS + sub, COLS), COLS)
            out = fdot(m_buf[...], jnp.concatenate([part[:rows, sub:sub + COLS] for part, rows in zip(parts, dn_rows)], axis=0))
            z_buf[lax.rem(blk, 2), :, sub:sub + COLS] = (h_buf[:, cols].astype(F32) + out).astype(BF16)
        z_copy(blk).start()
        for idx in range(len(dn_rows)):
            issue(num + idx + SLOTS)

    for blk in range(max(0, n_dn - 2), n_dn):
        z_copy(blk).wait()


def solution(mesh):
    cp_size = mesh.shape['cp']
    side = math.isqrt(cp_size // 2)
    vmem = pl.BlockSpec(memory_space=pltpu.VMEM)
    hbm = pl.BlockSpec(memory_space=pl.ANY)
    dma = pltpu.SemaphoreType.DMA
    limit = 60 * 1024 * 1024

    def device_fn(x_loc, seg_loc, pos_loc, attn_gain, w_q, w_k, w_v, w_o, mlp_gain, w_gate, w_up, w_down):
        rows = x_loc[0]
        count, depth = rows.shape
        piece = count // 2
        width = w_q.shape[1] // HEAD_DIM * piece
        ff = w_gate.shape[1]
        pos3 = pos_loc.reshape(2, 1, piece)
        freqs = jnp.asarray(rope_freqs()).reshape(HEAD_DIM // 2, 1)
        chunks = depth // SLOT_ROWS
        blocks = count // 32
        table = jax.ShapeDtypeStruct((count, HEAD_DIM), F32)
        cache = jax.ShapeDtypeStruct((count, HEAD_DIM), BF16)
        a_rows, cos_t, sin_t, kv, k_rows, v_rows = pl.pallas_call(
            project_kernel,
            out_shape=(jax.ShapeDtypeStruct((count, depth), BF16), table, table, jax.ShapeDtypeStruct((4, piece, HEAD_DIM), BF16), cache, cache),
            in_specs=[hbm, vmem, vmem, vmem, hbm, hbm],
            out_specs=(hbm, vmem, vmem, vmem, vmem, vmem),
            scratch_shapes=[pltpu.VMEM((count, depth), BF16), pltpu.VMEM((count, depth), BF16), pltpu.VMEM((depth, HEAD_DIM), BF16), pltpu.VMEM((depth, HEAD_DIM), BF16), dma((blocks,)), dma((2,)), dma((blocks,))],
            compiler_params=pltpu.CompilerParams(vmem_limit_bytes=limit),
            name='project',
        )(rows, attn_gain, pos3, freqs, w_k, w_v)
        attn_rows = pl.pallas_call(
            functools.partial(attend_kernel, cp_size, side),
            out_shape=jax.ShapeDtypeStruct((count, w_q.shape[1]), BF16),
            in_specs=[vmem, vmem, vmem, vmem, hbm, hbm],
            out_specs=vmem,
            scratch_shapes=[pltpu.VMEM((count, depth), BF16), pltpu.VMEM((chunks, SLOT_ROWS, w_q.shape[1]), BF16), pltpu.VMEM((2, HEAD_DIM, width), BF16), pltpu.VMEM((cp_size, 4, piece, HEAD_DIM), BF16), pltpu.VMEM((2, 1, width), F32), pltpu.VMEM((2, 1, width), F32), pltpu.VMEM((2, HEAD_DIM, width), F32), pltpu.VMEM((OWNERS * piece, LANES), F32), dma(()), dma((chunks,)), dma((NUM_COPIES,)), dma((NUM_COPIES,))],
            compiler_params=pltpu.CompilerParams(vmem_limit_bytes=limit, collective_id=0, has_side_effects=True),
            name='attend',
        )(kv, pos3, cos_t, sin_t, a_rows, w_q)
        z_rows = pl.pallas_call(
            finish_kernel,
            out_shape=jax.ShapeDtypeStruct((count, depth), BF16),
            in_specs=[hbm, vmem, vmem, hbm, hbm, hbm, hbm],
            out_specs=hbm,
            scratch_shapes=[pltpu.VMEM((count, depth), BF16), pltpu.VMEM((count, depth), BF16), pltpu.VMEM((count, ff), BF16), pltpu.VMEM((2, count, ff // 2), F32), pltpu.VMEM((2, count, SLOT_COLS), BF16), pltpu.VMEM((SLOTS, SLOT_ROWS, SLOT_COLS), BF16), dma(()), dma((SLOTS,)), dma((2,))],
            compiler_params=pltpu.CompilerParams(vmem_limit_bytes=limit),
            name='finish',
        )(rows, attn_rows, mlp_gain, w_o, w_gate, w_up, w_down)
        return z_rows[None], k_rows[:, None, :], v_rows[:, None, :]

    seq_spec = P(('dp', 'cp'))
    return jax.shard_map(device_fn, mesh=mesh, in_specs=(P('dp', 'cp', None), seq_spec, seq_spec, P(), P(), P(), P(), P(), P(), P(), P(), P()), out_specs=(P('dp', 'cp', None), P(('dp', 'cp'), None, None), P(('dp', 'cp'), None, None)), check_vma=False)
```

```python
import functools
import math

import jax
import jax.numpy as jnp
import numpy as np
from jax import lax
from jax.experimental import pallas as pl
from jax.experimental.pallas import tpu as pltpu
from jax.sharding import PartitionSpec as P

HEAD_DIM = 128
ROPE_THETA = 500000.0
ROPE_FACTOR = 8.0
LOW_FREQ = 1.0
HIGH_FREQ = 4.0
ORIG_CTX = 8192.0
NORM_EPS = 1e-5
NEG_BIG = -1e30
SCORE_LOG2 = HEAD_DIM ** -0.5 * math.log2(math.e)
MESH = pl.DeviceIdType.MESH
COLS = 512
SLOTS = 6
SLOT_ROWS = 1024
SLOT_COLS = 2048
OWNERS = 4
LANES = 256
F32 = jnp.float32
BF16 = jnp.bfloat16


def rope_freqs():
    exponent = np.arange(0, HEAD_DIM, 2) / HEAD_DIM
    inv_freq = 1.0 / (ROPE_THETA ** exponent)
    wavelen = 2.0 * np.pi / inv_freq
    smooth = np.clip((ORIG_CTX / wavelen - LOW_FREQ) / (HIGH_FREQ - LOW_FREQ), 0.0, 1.0)
    return ((1.0 - smooth) * inv_freq / ROPE_FACTOR + smooth * inv_freq).astype(np.float32)


def fdot(lhs, rhs):
    return jnp.dot(lhs, rhs, preferred_element_type=F32)


def norm_rows(src_ref, dst_ref, gain_ref, row, count):
    depth = src_ref.shape[1]
    rows = pl.ds(row, count)
    total = jnp.zeros((count, 128), F32)
    for col in range(0, depth, 128):
        part = src_ref[rows, col:col + 128].astype(F32)
        total = total + part * part
    inv_rms = lax.rsqrt(jnp.sum(total, axis=1, keepdims=True) / depth + NORM_EPS)
    for col in range(0, depth, 512):
        part = src_ref[rows, col:col + 512].astype(F32)
        gain = gain_ref[col:col + 512].astype(F32).reshape(1, 512)
        dst_ref[rows, col:col + 512] = (part * inv_rms * gain).astype(BF16)


def project_kernel(x_hbm, gain_ref, pos_ref, freq_ref, wk_hbm, wv_hbm, a_hbm, cos_ref, sin_ref, kv_ref, pos_out, kc_ref, vc_ref, x_buf, a_buf, wk_buf, wv_buf, x_sem, wkv_sem, a_sem):
    count = x_buf.shape[0]
    piece = count // 2
    blocks = x_sem.shape[0]
    rows_blk = count // blocks

    def x_copy(idx):
        rows = pl.ds(idx * rows_blk, rows_blk)
        return pltpu.make_async_copy(x_hbm.at[rows], x_buf.at[rows], x_sem.at[idx])

    def a_copy(idx):
        rows = pl.ds(idx * rows_blk, rows_blk)
        return pltpu.make_async_copy(a_buf.at[rows], a_hbm.at[rows], a_sem.at[idx])

    for idx in range(blocks):
        x_copy(idx).start()
    wkv = [pltpu.make_async_copy(wk_hbm, wk_buf, wkv_sem.at[0]), pltpu.make_async_copy(wv_hbm, wv_buf, wkv_sem.at[1])]
    for copy in wkv:
        copy.start(priority=1)
    pos_out[...] = pos_ref[...]
    for half in range(2):
        rows = slice(half * piece, (half + 1) * piece)
        angles = freq_ref[...] * pos_ref[half].astype(F32)
        cos_h = jnp.cos(angles).T
        sin_h = jnp.sin(angles).T
        cos_ref[rows] = jnp.concatenate([cos_h, cos_h], axis=1)
        sin_ref[rows] = jnp.concatenate([-sin_h, sin_h], axis=1)

    @pl.loop(0, blocks)
    def _(idx):
        x_copy(idx).wait()
        norm_rows(x_buf, a_buf, gain_ref, pl.multiple_of(idx * rows_blk, rows_blk), rows_blk)
        a_copy(idx).start()

    for copy in wkv:
        copy.wait()
    kv_raw = fdot(a_buf[...], jnp.concatenate([wk_buf[...], wv_buf[...]], axis=1))
    k_rot = rope(kv_raw[:, :HEAD_DIM], cos_ref[...], sin_ref[...])
    v_raw = kv_raw[:, HEAD_DIM:]
    kc_ref[...] = k_rot.astype(BF16)
    vc_ref[...] = v_raw.astype(BF16)
    for half in range(2):
        rows = slice(half * piece, (half + 1) * piece)
        kv_ref[half] = k_rot[rows].astype(BF16)
        kv_ref[2 + half] = v_raw[rows].T.astype(BF16)
    for idx in range(blocks):
        a_copy(idx).wait()


def rope(raw, cos_t, sin_t):
    half = HEAD_DIM // 2
    return raw * cos_t + jnp.concatenate([raw[:, half:], raw[:, :half]], axis=1) * sin_t


def torus_place(side):
    me = lax.axis_index('cp')
    core = lax.rem(me, 2)
    chip = me // 2
    chip_x = lax.rem(chip, side)
    chip_y = chip // side

    def owner(first, second, core=core):
        pos_x = lax.rem(chip_x + first * (1 - core) + second * core + 2 * side, side)
        pos_y = lax.rem(chip_y + first * core + second * (1 - core) + 2 * side, side)
        return (pos_y * side + pos_x) * 2 + core

    def other(first, second):
        return owner(first, second, 1 - core)

    return me, owner, other


def gather_shards(place, kv_ref, all_ref, send_sem, recv_sem, on_start, on_group):
    me, owner, other = place
    sibling = other(0, 0)
    targets = {'a+': owner(1, 0), 'a-': owner(-1, 0), 'b+': owner(0, 1), 'b-': owner(0, -1), 's': sibling}
    barrier = pltpu.get_barrier_semaphore()
    for target in targets.values():
        pl.semaphore_signal(barrier, inc=1, device_id={'cp': target}, device_id_type=MESH)
    pl.semaphore_wait(barrier, len(targets))

    copies = []

    def send(shard, where, half=None):
        num = len(copies)
        dst = all_ref.at[shard]
        src = kv_ref if num < 5 else dst
        if half is not None:
            dst = dst.at[pl.ds(2 * half, 2)]
            src = dst
        copy = pltpu.make_async_remote_copy(src_ref=src, dst_ref=dst, send_sem=send_sem.at[num], recv_sem=recv_sem.at[num], device_id={'cp': targets[where]}, device_id_type=MESH)
        copy.start()
        copies.append(copy)
        return copy

    from_sibling = []

    def spread(shard):
        plus = send(shard, 'b+')
        minus = send(shard, 'b-')
        from_sibling.append(send(shard, 's'))
        return plus, minus

    def relay(first, row):
        row[0].wait_recv()
        shard = owner(first, -1)
        half_k = send(shard, 'b+', 0)
        from_sibling.append(send(shard, 's'))
        row[1].wait_recv()
        shard = owner(first, 1)
        half_v = send(shard, 'b-', 1)
        from_sibling.append(send(shard, 's'))
        return half_k, half_v

    def close(first, halves):
        halves[0].wait_recv()
        halves[1].wait_recv()
        from_sibling.append(send(owner(first, 2), 's'))

    def arrived(*nums):
        for num in nums:
            from_sibling[num].wait_recv()

    own_right = send(me, 'a+')
    own_left = send(me, 'a-')
    row_own = spread(me)
    all_ref[me] = kv_ref[...]
    own_right.wait_recv()
    shard = owner(-1, 0)
    far_k = send(shard, 'a+', 0)
    row_left = spread(shard)
    own_left.wait_recv()
    shard = owner(1, 0)
    far_v = send(shard, 'a-', 1)
    row_right = spread(shard)
    far_own = relay(0, row_own)
    on_start(0)
    far_k.wait_recv()
    far_v.wait_recv()
    row_far = spread(owner(2, 0))
    on_start(1)
    far_left = relay(-1, row_left)
    far_right = relay(1, row_right)
    arrived(0)
    on_group(me, sibling, owner(-1, 0), owner(1, 0))
    close(0, far_own)
    far_far = relay(2, row_far)
    arrived(1, 2)
    on_group(owner(0, -1), owner(0, 1), other(-1, 0), other(1, 0))
    close(-1, far_left)
    close(1, far_right)
    arrived(3, 4)
    on_group(owner(2, 0), owner(-1, -1), other(0, -1), other(0, 1))
    close(2, far_far)
    arrived(5)
    on_group(owner(-1, 1), owner(1, -1), owner(1, 1), other(2, 0))
    arrived(6, 7)
    on_group(owner(0, 2), owner(2, -1), other(-1, -1), other(-1, 1))
    arrived(8, 9)
    on_group(owner(2, 1), owner(-1, 2), other(1, -1), other(1, 1))
    arrived(10, 11)
    on_group(owner(1, 2), owner(2, 2), other(0, 2), other(2, -1))
    arrived(12, 13, 14, 15)
    on_group(other(2, 1), other(-1, 2), other(1, 2), other(2, 2))
    for copy in copies:
        copy.wait_send()


NUM_COPIES = 36


def attend_kernel(cp_size, side, kv_ref, pos_ref, cos_ref, sin_ref, a_hbm, wq_hbm, wo_hbm, out_ref, wo_ref, a_buf, wq_buf, qt_ref, all_ref, max_ref, sum_ref, acc_ref, score_ref, a_sem, wq_sem, wo_sem, send_sem, recv_sem):
    place = torus_place(side)
    me = place[0]
    count = a_buf.shape[0]
    piece = count // 2
    width = qt_ref.shape[2]
    tiles = width // LANES
    chunks, chunk_rows = wq_buf.shape[:2]
    loads = [pltpu.make_async_copy(a_hbm, a_buf, a_sem)]
    loads += [pltpu.make_async_copy(wq_hbm.at[pl.ds(idx * chunk_rows, chunk_rows)], wq_buf.at[idx], wq_sem.at[idx]) for idx in range(chunks)]
    wo_copy = pltpu.make_async_copy(wo_hbm, wo_ref, wo_sem)
    for copy in loads + [wo_copy]:
        copy.start()

    bases = (me * piece, (2 * cp_size - 1 - me) * piece)
    lane_tok = lax.broadcasted_iota(jnp.int32, (1, piece), 1)

    def starts(half):
        first = bases[half] + lane_tok - pos_ref[half]
        return jnp.concatenate([first] * (LANES // piece), axis=1)

    first_key = (starts(0), starts(1))
    tok = jnp.concatenate([lane_tok] * (LANES // piece), axis=1)
    key_row = lax.broadcasted_iota(jnp.int32, (piece, LANES), 0)

    n_blocks = wq_buf.shape[2] // COLS

    def queries(part):
        if part == 0:
            for copy in loads:
                copy.wait()
        for col in range(part * n_blocks // 2, (part + 1) * n_blocks // 2):
            q_raw = fdot(a_buf[...], jnp.concatenate([wq_buf[idx, :, col * COLS:(col + 1) * COLS] for idx in range(chunks)], axis=0))
            for sub in range(COLS // HEAD_DIM):
                head = col * (COLS // HEAD_DIM) + sub
                q_rot = rope(q_raw[:, sub * HEAD_DIM:(sub + 1) * HEAD_DIM], cos_ref[...], sin_ref[...])
                for half in range(2):
                    qt_ref[half, :, head * piece:(head + 1) * piece] = q_rot[half * piece:(half + 1) * piece].T.astype(BF16)
        if part == 1:
            for half in range(2):
                visible = (key_row <= tok) & (key_row + bases[half] >= first_key[half])
                for tile in range(tiles):
                    cols = slice(tile * LANES, (tile + 1) * LANES)
                    scores = fdot(kv_ref[half], qt_ref[half, :, cols])
                    scores = jnp.where(visible, scores, NEG_BIG)
                    top = jnp.max(scores, axis=0, keepdims=True)
                    prob = jnp.exp2((scores - top) * SCORE_LOG2)
                    max_ref[half, :, cols] = top
                    sum_ref[half, :, cols] = jnp.sum(prob, axis=0, keepdims=True)
                    acc_ref[half, :, cols] = fdot(kv_ref[2 + half], prob.astype(BF16))

    def block(half, part, owners, key_base):
        keys = jnp.concatenate([all_ref[own, part] for own in owners], axis=0)
        vals = jnp.concatenate([all_ref[own, 2 + part] for own in owners], axis=1)
        hidden = [key_row < first_key[half] - base for base in key_base]
        tops, scales = [], []
        for tile in range(tiles):
            cols = slice(tile * LANES, (tile + 1) * LANES)
            raw = fdot(keys, qt_ref[half, :, cols])
            peak = None
            for sub in range(OWNERS):
                rows = slice(sub * piece, (sub + 1) * piece)
                score = jnp.where(hidden[sub], NEG_BIG, raw[rows])
                score_ref[rows, cols] = score
                best = jnp.max(score, axis=0, keepdims=True)
                peak = best if peak is None else jnp.maximum(peak, best)
            old_top = max_ref[half, :, cols]
            top = jnp.maximum(old_top, peak)
            max_ref[half, :, cols] = top
            tops.append(top)
            scales.append(jnp.exp2((old_top - top) * SCORE_LOG2))
        for tile in range(tiles):
            cols = slice(tile * LANES, (tile + 1) * LANES)
            prob = jnp.exp2((score_ref[:, cols] - tops[tile]) * SCORE_LOG2)
            sum_ref[half, :, cols] = sum_ref[half, :, cols] * scales[tile] + jnp.sum(prob, axis=0, keepdims=True)
            acc_ref[half, :, cols] = acc_ref[half, :, cols] * scales[tile] + fdot(vals, prob.astype(BF16))

    def low_group(*owners):
        block(1, 0, owners, [own * piece for own in owners])

    gather_shards(place, kv_ref, all_ref, send_sem, recv_sem, queries, low_group)

    @pl.loop(0, (me + OWNERS - 1) // OWNERS)
    def _(idx):
        owners = [idx * OWNERS + sub for sub in range(OWNERS)]
        block(0, 0, owners, [jnp.where(own < me, own * piece, -2 * piece) for own in owners])

    @pl.loop((me + 1) // OWNERS, cp_size // OWNERS)
    def _(idx):
        owners = [idx * OWNERS + sub for sub in range(OWNERS)]
        block(1, 1, owners, [jnp.where(own > me, (2 * cp_size - 1 - own) * piece, -2 * piece) for own in owners])

    for half in range(2):
        for head in range(width // piece):
            cols = slice(head * piece, (head + 1) * piece)
            done = acc_ref[half, :, cols] / sum_ref[half, :, cols]
            out_ref[half * piece:(half + 1) * piece, head * HEAD_DIM:(head + 1) * HEAD_DIM] = done.T.astype(BF16)
    wo_copy.wait()


def finish_kernel(x_hbm, attn_ref, gain_ref, wo_ref, wg_hbm, wu_hbm, wd_hbm, z_hbm, h_buf, b_buf, m_buf, acc_ref, z_buf, slots, x_sem, slot_sem, z_sem):
    count, depth = h_buf.shape
    ff = wg_hbm.shape[1]
    ff_half = ff // 2
    group = 2
    n_wo = depth // SLOT_COLS
    k_steps = depth // (SLOT_ROWS * group)
    n_ff = 4 * k_steps
    dn_cols = SLOT_COLS // 2
    dn_rows = [min(SLOT_ROWS, ff - row) for row in range(0, ff, SLOT_ROWS)]
    dn_slots = [dn_rows[idx:idx + 2] for idx in range(0, len(dn_rows), 2)]
    n_dn = depth // dn_cols
    ff_from = 0
    dn_from = ff_from + n_ff * group
    total = dn_from + n_dn * len(dn_slots)

    def cols_of(idx, size):
        return pl.ds(pl.multiple_of(idx * size, size), size)

    def halves(src, dst, rows, sem):
        for part in range(2):
            sel = pl.ds(part * rows // 2, rows // 2)
            pltpu.make_async_copy(src.at[sel], dst.at[sel], sem).start(priority=part)

    def issue(num):
        slot = lax.rem(num, SLOTS)
        sem = slot_sem.at[slot]
        dst = slots.at[slot]

        rel = num - ff_from
        step = rel // group
        half = step // (2 * k_steps)
        kind = lax.rem(step // k_steps, 2)
        row = cols_of(lax.rem(step, k_steps) * group + lax.rem(rel, group), SLOT_ROWS)
        in_ff = (num >= ff_from) & (num < dn_from)

        @pl.when(in_ff & (kind == 0))
        def _():
            halves(wg_hbm.at[row, cols_of(half, ff_half)], dst.at[:, pl.ds(0, ff_half)], SLOT_ROWS, sem)

        @pl.when(in_ff & (kind == 1))
        def _():
            halves(wu_hbm.at[row, cols_of(half, ff_half)], dst.at[:, pl.ds(0, ff_half)], SLOT_ROWS, sem)

        rel = num - dn_from
        for idx, pair in enumerate(dn_slots):
            @pl.when((num >= dn_from) & (num < total) & (lax.rem(rel, len(dn_slots)) == idx))
            def _():
                for side, rows in enumerate(pair):
                    src = wd_hbm.at[pl.ds((2 * idx + side) * SLOT_ROWS, rows), cols_of(rel // len(dn_slots), dn_cols)]
                    pltpu.make_async_copy(src, dst.at[pl.ds(0, rows), pl.ds(side * dn_cols, dn_cols)], sem).start(priority=side)

    def take(num, rows, cols):
        slot = lax.rem(num, SLOTS)
        part = slots.at[slot, pl.ds(0, rows), pl.ds(0, cols)]
        pltpu.make_async_copy(part, part, slot_sem.at[slot]).wait()
        return slots.at[slot]

    x_copy = pltpu.make_async_copy(x_hbm, h_buf, x_sem)
    x_copy.start()
    for num in range(SLOTS):
        issue(jnp.int32(num))
    x_copy.wait()

    @pl.loop(0, n_wo)
    def _(num):
        for sub in range(0, SLOT_COLS, COLS):
            cols = pl.ds(pl.multiple_of(num * SLOT_COLS + sub, COLS), COLS)
            out = fdot(attn_ref[...], wo_ref[:, cols])
            h_buf[:, cols] = (h_buf[:, cols].astype(F32) + out).astype(BF16)

    @pl.loop(0, count // 32)
    def _(idx):
        norm_rows(h_buf, b_buf, gain_ref, pl.multiple_of(idx * 32, 32), 32)

    @pl.loop(0, n_ff)
    def _(step):
        num = ff_from + step * group
        half = step // (2 * k_steps)
        kind = lax.rem(step // k_steps, 2)
        k_idx = lax.rem(step, k_steps)
        parts = [take(num + sub, SLOT_ROWS, ff_half) for sub in range(group)]
        lhs = b_buf[:, cols_of(k_idx, SLOT_ROWS * group)]
        for col in range(0, ff_half, COLS):
            size = min(COLS, ff_half - col)
            cols = slice(col, col + size)
            out = fdot(lhs, jnp.concatenate([part[:, cols] for part in parts], axis=0))
            acc_ref[kind, :, cols] = jnp.where(k_idx == 0, 0.0, acc_ref[kind, :, cols]) + out
        for sub in range(group):
            issue(num + sub + SLOTS)

        @pl.when((kind == 1) & (k_idx == k_steps - 1))
        def _():
            for col in range(0, ff_half, 256):
                gate = acc_ref[0, :, col:col + 256]
                dst = pl.ds(pl.multiple_of(half * ff_half + col, 256), 256)
                m_buf[:, dst] = (gate * jax.nn.sigmoid(gate) * acc_ref[1, :, col:col + 256]).astype(BF16)

    def z_copy(blk):
        slot = lax.rem(blk, 2)
        return pltpu.make_async_copy(z_buf.at[slot], z_hbm.at[:, cols_of(blk, dn_cols)], z_sem.at[slot])

    @pl.loop(0, n_dn)
    def _(blk):
        num = dn_from + blk * len(dn_slots)
        parts = []
        for idx, pair in enumerate(dn_slots):
            slot = lax.rem(num + idx, SLOTS)
            for side, rows in enumerate(pair):
                part = slots.at[slot, pl.ds(0, rows), pl.ds(side * dn_cols, dn_cols)]
                pltpu.make_async_copy(part, part, slot_sem.at[slot]).wait()
                parts.append(part)

        @pl.when(blk >= 2)
        def _():
            z_copy(blk - 2).wait()

        for sub in range(0, dn_cols, COLS):
            cols = pl.ds(pl.multiple_of(blk * dn_cols + sub, COLS), COLS)
            out = fdot(m_buf[...], jnp.concatenate([part[:, sub:sub + COLS] for part in parts], axis=0))
            z_buf[lax.rem(blk, 2), :, sub:sub + COLS] = (h_buf[:, cols].astype(F32) + out).astype(BF16)
        z_copy(blk).start()
        for idx in range(len(dn_slots)):
            issue(num + idx + SLOTS)

    for blk in range(max(0, n_dn - 2), n_dn):
        z_copy(blk).wait()


def in_vmem(array):
    return pltpu.with_memory_space_constraint(array, pltpu.VMEM)


def solution(mesh):
    cp_size = mesh.shape['cp']
    side = math.isqrt(cp_size // 2)
    vmem = pl.BlockSpec(memory_space=pltpu.VMEM)
    hbm = pl.BlockSpec(memory_space=pl.ANY)
    dma = pltpu.SemaphoreType.DMA
    limit = 60 * 1024 * 1024

    def device_fn(x_loc, seg_loc, pos_loc, attn_gain, w_q, w_k, w_v, w_o, mlp_gain, w_gate, w_up, w_down):
        rows = x_loc[0]
        count, depth = rows.shape
        piece = count // 2
        width = w_q.shape[1] // HEAD_DIM * piece
        ff = w_gate.shape[1]
        pos3 = pos_loc.reshape(2, 1, piece)
        freqs = jnp.asarray(rope_freqs()).reshape(HEAD_DIM // 2, 1)
        chunks = depth // SLOT_ROWS
        blocks = count // 32
        table = jax.ShapeDtypeStruct((count, HEAD_DIM), F32)
        cache = jax.ShapeDtypeStruct((count, HEAD_DIM), BF16)
        a_rows, cos_t, sin_t, kv, pos_v, k_rows, v_rows = pl.pallas_call(
            project_kernel,
            out_shape=(jax.ShapeDtypeStruct((count, depth), BF16), table, table, jax.ShapeDtypeStruct((4, piece, HEAD_DIM), BF16), jax.ShapeDtypeStruct((2, 1, piece), jnp.int32), cache, cache),
            in_specs=[hbm, vmem, vmem, vmem, hbm, hbm],
            out_specs=(hbm, vmem, vmem, vmem, vmem, vmem, vmem),
            scratch_shapes=[pltpu.VMEM((count, depth), BF16), pltpu.VMEM((count, depth), BF16), pltpu.VMEM((depth, HEAD_DIM), BF16), pltpu.VMEM((depth, HEAD_DIM), BF16), dma((blocks,)), dma((2,)), dma((blocks,))],
            compiler_params=pltpu.CompilerParams(vmem_limit_bytes=24 * 1024 * 1024),
            name='project',
        )(rows, attn_gain, pos3, freqs, w_k, w_v)
        attn_rows, wo_near = pl.pallas_call(
            functools.partial(attend_kernel, cp_size, side),
            out_shape=(jax.ShapeDtypeStruct((count, w_q.shape[1]), BF16), jax.ShapeDtypeStruct(w_o.shape, BF16)),
            in_specs=[vmem, vmem, vmem, vmem, hbm, hbm, hbm],
            out_specs=(vmem, vmem),
            scratch_shapes=[pltpu.VMEM((count, depth), BF16), pltpu.VMEM((chunks, SLOT_ROWS, w_q.shape[1]), BF16), pltpu.VMEM((2, HEAD_DIM, width), BF16), pltpu.VMEM((cp_size, 4, piece, HEAD_DIM), BF16), pltpu.VMEM((2, 1, width), F32), pltpu.VMEM((2, 1, width), F32), pltpu.VMEM((2, HEAD_DIM, width), F32), pltpu.VMEM((OWNERS * piece, width), F32), dma(()), dma((chunks,)), dma(()), dma((NUM_COPIES,)), dma((NUM_COPIES,))],
            compiler_params=pltpu.CompilerParams(vmem_limit_bytes=36 * 1024 * 1024, collective_id=0, has_side_effects=True),
            name='attend',
        )(in_vmem(kv), in_vmem(pos_v), in_vmem(cos_t), in_vmem(sin_t), pltpu.with_memory_space_constraint(a_rows, pltpu.HBM), pltpu.with_memory_space_constraint(w_q, pltpu.HBM), pltpu.with_memory_space_constraint(w_o, pltpu.HBM))
        z_rows = pl.pallas_call(
            finish_kernel,
            out_shape=jax.ShapeDtypeStruct((count, depth), BF16),
            in_specs=[hbm, vmem, vmem, vmem, hbm, hbm, hbm],
            out_specs=hbm,
            scratch_shapes=[pltpu.VMEM((count, depth), BF16), pltpu.VMEM((count, depth), BF16), pltpu.VMEM((count, ff), BF16), pltpu.VMEM((2, count, ff // 2), F32), pltpu.VMEM((2, count, SLOT_COLS // 2), BF16), pltpu.VMEM((SLOTS, SLOT_ROWS, SLOT_COLS), BF16), dma(()), dma((SLOTS,)), dma((2,))],
            compiler_params=pltpu.CompilerParams(vmem_limit_bytes=42 * 1024 * 1024),
            name='finish',
        )(rows, in_vmem(attn_rows), mlp_gain, in_vmem(wo_near), w_gate, w_up, w_down)
        return z_rows[None], k_rows[:, None, :], v_rows[:, None, :]

    seq_spec = P(('dp', 'cp'))
    return jax.shard_map(device_fn, mesh=mesh, in_specs=(P('dp', 'cp', None), seq_spec, seq_spec, P(), P(), P(), P(), P(), P(), P(), P(), P()), out_specs=(P('dp', 'cp', None), P(('dp', 'cp'), None, None), P(('dp', 'cp'), None, None)), check_vma=False)
```

```python
import functools
import math

import jax
import jax.numpy as jnp
import numpy as np
from jax import lax
from jax.experimental import pallas as pl
from jax.experimental.pallas import tpu as pltpu
from jax.sharding import PartitionSpec as P

HEAD_DIM = 128
ROPE_THETA = 500000.0
ROPE_FACTOR = 8.0
LOW_FREQ = 1.0
HIGH_FREQ = 4.0
ORIG_CTX = 8192.0
NORM_EPS = 1e-5
NEG_BIG = -1e30
SCORE_LOG2 = HEAD_DIM ** -0.5 * math.log2(math.e)
MESH = pl.DeviceIdType.MESH
COLS = 512
SLOTS = 6
SLOT_ROWS = 1024
SLOT_COLS = 2048
OWNERS = 4
LANES = 256
F32 = jnp.float32
BF16 = jnp.bfloat16


def rope_freqs():
    exponent = np.arange(0, HEAD_DIM, 2) / HEAD_DIM
    inv_freq = 1.0 / (ROPE_THETA ** exponent)
    wavelen = 2.0 * np.pi / inv_freq
    smooth = np.clip((ORIG_CTX / wavelen - LOW_FREQ) / (HIGH_FREQ - LOW_FREQ), 0.0, 1.0)
    return ((1.0 - smooth) * inv_freq / ROPE_FACTOR + smooth * inv_freq).astype(np.float32)


def fdot(lhs, rhs):
    return jnp.dot(lhs, rhs, preferred_element_type=F32)


def norm_rows(src_ref, dst_ref, gain_ref, row, count):
    depth = src_ref.shape[1]
    rows = pl.ds(row, count)
    total = jnp.zeros((count, 128), F32)
    for col in range(0, depth, 128):
        part = src_ref[rows, col:col + 128].astype(F32)
        total = total + part * part
    inv_rms = lax.rsqrt(jnp.sum(total, axis=1, keepdims=True) / depth + NORM_EPS)
    for col in range(0, depth, 512):
        part = src_ref[rows, col:col + 512].astype(F32)
        gain = gain_ref[col:col + 512].astype(F32).reshape(1, 512)
        dst_ref[rows, col:col + 512] = (part * inv_rms * gain).astype(BF16)


def project_kernel(x_hbm, gain_ref, pos_ref, freq_ref, wk_hbm, wv_hbm, a_buf, cos_ref, sin_ref, kv_ref, pos_out, kc_ref, vc_ref, x_buf, wk_buf, wv_buf, x_sem, wkv_sem):
    count = x_buf.shape[0]
    piece = count // 2
    blocks = x_sem.shape[0]
    rows_blk = count // blocks

    def x_copy(idx):
        rows = pl.ds(idx * rows_blk, rows_blk)
        return pltpu.make_async_copy(x_hbm.at[rows], x_buf.at[rows], x_sem.at[idx])

    for idx in range(blocks):
        x_copy(idx).start()
    wkv = [pltpu.make_async_copy(wk_hbm, wk_buf, wkv_sem.at[0]), pltpu.make_async_copy(wv_hbm, wv_buf, wkv_sem.at[1])]
    for copy in wkv:
        copy.start(priority=1)
    pos_out[...] = pos_ref[...]
    for half in range(2):
        rows = slice(half * piece, (half + 1) * piece)
        angles = freq_ref[...] * pos_ref[half].astype(F32)
        cos_h = jnp.cos(angles).T
        sin_h = jnp.sin(angles).T
        cos_ref[rows] = jnp.concatenate([cos_h, cos_h], axis=1)
        sin_ref[rows] = jnp.concatenate([-sin_h, sin_h], axis=1)

    @pl.loop(0, blocks)
    def _(idx):
        x_copy(idx).wait()
        norm_rows(x_buf, a_buf, gain_ref, pl.multiple_of(idx * rows_blk, rows_blk), rows_blk)

    for copy in wkv:
        copy.wait()
    kv_raw = fdot(a_buf[...], jnp.concatenate([wk_buf[...], wv_buf[...]], axis=1))
    k_rot = rope(kv_raw[:, :HEAD_DIM], cos_ref[...], sin_ref[...])
    v_raw = kv_raw[:, HEAD_DIM:]
    kc_ref[...] = k_rot.astype(BF16)
    vc_ref[...] = v_raw.astype(BF16)
    for half in range(2):
        rows = slice(half * piece, (half + 1) * piece)
        kv_ref[half] = k_rot[rows].astype(BF16)
        kv_ref[2 + half] = v_raw[rows].T.astype(BF16)


def rope(raw, cos_t, sin_t):
    half = HEAD_DIM // 2
    return raw * cos_t + jnp.concatenate([raw[:, half:], raw[:, :half]], axis=1) * sin_t


def torus_place(side):
    me = lax.axis_index('cp')
    core = lax.rem(me, 2)
    chip = me // 2
    chip_x = lax.rem(chip, side)
    chip_y = chip // side

    def owner(first, second, core=core):
        pos_x = lax.rem(chip_x + first * (1 - core) + second * core + 2 * side, side)
        pos_y = lax.rem(chip_y + first * core + second * (1 - core) + 2 * side, side)
        return (pos_y * side + pos_x) * 2 + core

    def other(first, second):
        return owner(first, second, 1 - core)

    return me, owner, other


def gather_shards(place, kv_ref, all_ref, send_sem, recv_sem, on_start, on_group):
    me, owner, other = place
    sibling = other(0, 0)
    targets = {'a+': owner(1, 0), 'a-': owner(-1, 0), 'b+': owner(0, 1), 'b-': owner(0, -1), 's': sibling}
    barrier = pltpu.get_barrier_semaphore()
    for target in targets.values():
        pl.semaphore_signal(barrier, inc=1, device_id={'cp': target}, device_id_type=MESH)
    pl.semaphore_wait(barrier, len(targets))

    copies = []

    def send(shard, where, half=None):
        num = len(copies)
        dst = all_ref.at[shard]
        src = kv_ref if num < 5 else dst
        if half is not None:
            dst = dst.at[pl.ds(2 * half, 2)]
            src = dst
        copy = pltpu.make_async_remote_copy(src_ref=src, dst_ref=dst, send_sem=send_sem.at[num], recv_sem=recv_sem.at[num], device_id={'cp': targets[where]}, device_id_type=MESH)
        copy.start()
        copies.append(copy)
        return copy

    from_sibling = []

    def spread(shard):
        plus = send(shard, 'b+')
        minus = send(shard, 'b-')
        from_sibling.append(send(shard, 's'))
        return plus, minus

    def relay(first, row):
        row[0].wait_recv()
        shard = owner(first, -1)
        half_k = send(shard, 'b+', 0)
        from_sibling.append(send(shard, 's'))
        row[1].wait_recv()
        shard = owner(first, 1)
        half_v = send(shard, 'b-', 1)
        from_sibling.append(send(shard, 's'))
        return half_k, half_v

    def close(first, halves):
        halves[0].wait_recv()
        halves[1].wait_recv()
        from_sibling.append(send(owner(first, 2), 's'))

    def arrived(*nums):
        for num in nums:
            from_sibling[num].wait_recv()

    own_right = send(me, 'a+')
    own_left = send(me, 'a-')
    row_own = spread(me)
    all_ref[me] = kv_ref[...]
    own_right.wait_recv()
    shard = owner(-1, 0)
    far_k = send(shard, 'a+', 0)
    row_left = spread(shard)
    own_left.wait_recv()
    shard = owner(1, 0)
    far_v = send(shard, 'a-', 1)
    row_right = spread(shard)
    far_own = relay(0, row_own)
    on_start(0)
    far_k.wait_recv()
    far_v.wait_recv()
    row_far = spread(owner(2, 0))
    on_start(1)
    far_left = relay(-1, row_left)
    far_right = relay(1, row_right)
    close(0, far_own)
    arrived(0)
    on_group(me, sibling, owner(-1, 0), owner(1, 0))
    far_far = relay(2, row_far)
    arrived(1, 2)
    on_group(owner(0, -1), owner(0, 1), other(-1, 0), other(1, 0))
    close(-1, far_left)
    close(1, far_right)
    arrived(3, 4)
    on_group(owner(2, 0), owner(-1, -1), other(0, -1), other(0, 1))
    close(2, far_far)
    arrived(5)
    on_group(owner(-1, 1), owner(1, -1), owner(1, 1), other(2, 0))
    arrived(6, 7)
    on_group(owner(0, 2), owner(2, -1), other(-1, -1), other(-1, 1))
    arrived(8, 9)
    on_group(owner(2, 1), owner(-1, 2), other(1, -1), other(1, 1))
    arrived(10, 11)
    on_group(owner(1, 2), owner(2, 2), other(0, 2), other(2, -1))
    arrived(12, 13, 14, 15)
    on_group(other(2, 1), other(-1, 2), other(1, 2), other(2, 2))
    for copy in copies:
        copy.wait_send()


NUM_COPIES = 36


def attend_kernel(cp_size, side, kv_ref, pos_ref, cos_ref, sin_ref, a_buf, wq_hbm, wo_hbm, out_ref, wo_ref, wq_buf, qt_ref, all_ref, max_ref, sum_ref, acc_ref, score_ref, wq_sem, wo_sem, send_sem, recv_sem):
    place = torus_place(side)
    me = place[0]
    count = a_buf.shape[0]
    piece = count // 2
    width = qt_ref.shape[2]
    tiles = width // LANES
    chunks, chunk_rows = wq_buf.shape[:2]
    loads = [pltpu.make_async_copy(wq_hbm.at[pl.ds(idx * chunk_rows, chunk_rows)], wq_buf.at[idx], wq_sem.at[idx]) for idx in range(chunks)]
    wo_copy = pltpu.make_async_copy(wo_hbm, wo_ref, wo_sem)
    for copy in loads + [wo_copy]:
        copy.start()

    bases = (me * piece, (2 * cp_size - 1 - me) * piece)
    lane_tok = lax.broadcasted_iota(jnp.int32, (1, piece), 1)

    def starts(half):
        first = bases[half] + lane_tok - pos_ref[half]
        return jnp.concatenate([first] * (LANES // piece), axis=1)

    first_key = (starts(0), starts(1))
    tok = jnp.concatenate([lane_tok] * (LANES // piece), axis=1)
    key_row = lax.broadcasted_iota(jnp.int32, (piece, LANES), 0)

    n_blocks = wq_buf.shape[2] // COLS

    def queries(part):
        if part == 0:
            for copy in loads:
                copy.wait()
        for col in range(part * n_blocks // 2, (part + 1) * n_blocks // 2):
            q_raw = fdot(a_buf[...], jnp.concatenate([wq_buf[idx, :, col * COLS:(col + 1) * COLS] for idx in range(chunks)], axis=0))
            for sub in range(COLS // HEAD_DIM):
                head = col * (COLS // HEAD_DIM) + sub
                q_rot = rope(q_raw[:, sub * HEAD_DIM:(sub + 1) * HEAD_DIM], cos_ref[...], sin_ref[...])
                for half in range(2):
                    qt_ref[half, :, head * piece:(head + 1) * piece] = q_rot[half * piece:(half + 1) * piece].T.astype(BF16)
        if part == 1:
            for half in range(2):
                visible = (key_row <= tok) & (key_row + bases[half] >= first_key[half])
                for tile in range(tiles):
                    cols = slice(tile * LANES, (tile + 1) * LANES)
                    scores = fdot(kv_ref[half], qt_ref[half, :, cols])
                    scores = jnp.where(visible, scores, NEG_BIG)
                    top = jnp.max(scores, axis=0, keepdims=True)
                    prob = jnp.exp2((scores - top) * SCORE_LOG2)
                    max_ref[half, :, cols] = top
                    sum_ref[half, :, cols] = jnp.sum(prob, axis=0, keepdims=True)
                    acc_ref[half, :, cols] = fdot(kv_ref[2 + half], prob.astype(BF16))

    def block(half, part, owners):
        start = jnp.where(half == 0, first_key[0], first_key[1])
        hidden = []
        for own in owners:
            low_base = jnp.where((half == 1) | (own < me), own * piece, -2 * piece)
            high_base = jnp.where(own > me, (2 * cp_size - 1 - own) * piece, -2 * piece)
            hidden.append(key_row < start - jnp.where(part == 0, low_base, high_base))
        keys = jnp.concatenate([all_ref[own, part] for own in owners], axis=0)
        vals = jnp.concatenate([all_ref[own, 2 + part] for own in owners], axis=1)
        tops, scales = [], []
        for tile in range(tiles):
            cols = slice(tile * LANES, (tile + 1) * LANES)
            raw = fdot(keys, qt_ref[half, :, cols])
            peak = None
            for sub in range(OWNERS):
                rows = slice(sub * piece, (sub + 1) * piece)
                score = jnp.where(hidden[sub], NEG_BIG, raw[rows])
                score_ref[rows, cols] = score
                best = jnp.max(score, axis=0, keepdims=True)
                peak = best if peak is None else jnp.maximum(peak, best)
            old_top = max_ref[half, :, cols]
            top = jnp.maximum(old_top, peak)
            max_ref[half, :, cols] = top
            tops.append(top)
            scales.append(jnp.exp2((old_top - top) * SCORE_LOG2))
        for tile in range(tiles):
            cols = slice(tile * LANES, (tile + 1) * LANES)
            prob = jnp.exp2((score_ref[:, cols] - tops[tile]) * SCORE_LOG2)
            sum_ref[half, :, cols] = sum_ref[half, :, cols] * scales[tile] + jnp.sum(prob, axis=0, keepdims=True)
            acc_ref[half, :, cols] = acc_ref[half, :, cols] * scales[tile] + fdot(vals, prob.astype(BF16))

    def on_group(*owners):
        @pl.loop(0, 3)
        def _(which):
            block((which + 1) // 2, which // 2, owners)

    gather_shards(place, kv_ref, all_ref, send_sem, recv_sem, queries, on_group)

    for half in range(2):
        for head in range(width // piece):
            cols = slice(head * piece, (head + 1) * piece)
            done = acc_ref[half, :, cols] / sum_ref[half, :, cols]
            out_ref[half * piece:(half + 1) * piece, head * HEAD_DIM:(head + 1) * HEAD_DIM] = done.T.astype(BF16)
    wo_copy.wait()


def finish_kernel(x_hbm, attn_ref, gain_ref, wo_ref, wg_hbm, wu_hbm, wd_hbm, z_hbm, h_buf, b_buf, m_buf, acc_ref, z_buf, slots, x_sem, slot_sem, z_sem):
    count, depth = h_buf.shape
    ff = wg_hbm.shape[1]
    ff_half = ff // 2
    group = 2
    n_wo = depth // SLOT_COLS
    k_steps = depth // (SLOT_ROWS * group)
    n_ff = 4 * k_steps
    dn_cols = SLOT_COLS // 2
    dn_rows = [min(SLOT_ROWS, ff - row) for row in range(0, ff, SLOT_ROWS)]
    dn_slots = [dn_rows[idx:idx + 2] for idx in range(0, len(dn_rows), 2)]
    n_dn = depth // dn_cols
    ff_from = 0
    dn_from = ff_from + n_ff * group
    total = dn_from + n_dn * len(dn_slots)

    def cols_of(idx, size):
        return pl.ds(pl.multiple_of(idx * size, size), size)

    def halves(src, dst, rows, sem):
        for part in range(2):
            sel = pl.ds(part * rows // 2, rows // 2)
            pltpu.make_async_copy(src.at[sel], dst.at[sel], sem).start(priority=part)

    def issue(num):
        slot = lax.rem(num, SLOTS)
        sem = slot_sem.at[slot]
        dst = slots.at[slot]

        rel = num - ff_from
        step = rel // group
        half = step // (2 * k_steps)
        kind = lax.rem(step // k_steps, 2)
        row = cols_of(lax.rem(step, k_steps) * group + lax.rem(rel, group), SLOT_ROWS)
        in_ff = (num >= ff_from) & (num < dn_from)

        @pl.when(in_ff & (kind == 0))
        def _():
            halves(wg_hbm.at[row, cols_of(half, ff_half)], dst.at[:, pl.ds(0, ff_half)], SLOT_ROWS, sem)

        @pl.when(in_ff & (kind == 1))
        def _():
            halves(wu_hbm.at[row, cols_of(half, ff_half)], dst.at[:, pl.ds(0, ff_half)], SLOT_ROWS, sem)

        rel = num - dn_from
        for idx, pair in enumerate(dn_slots):
            @pl.when((num >= dn_from) & (num < total) & (lax.rem(rel, len(dn_slots)) == idx))
            def _():
                for side, rows in enumerate(pair):
                    src = wd_hbm.at[pl.ds((2 * idx + side) * SLOT_ROWS, rows), cols_of(rel // len(dn_slots), dn_cols)]
                    pltpu.make_async_copy(src, dst.at[pl.ds(0, rows), pl.ds(side * dn_cols, dn_cols)], sem).start(priority=side)

    def take(num, rows, cols):
        slot = lax.rem(num, SLOTS)
        part = slots.at[slot, pl.ds(0, rows), pl.ds(0, cols)]
        pltpu.make_async_copy(part, part, slot_sem.at[slot]).wait()
        return slots.at[slot]

    x_copy = pltpu.make_async_copy(x_hbm, h_buf, x_sem)
    x_copy.start()
    for num in range(SLOTS):
        issue(jnp.int32(num))
    x_copy.wait()

    @pl.loop(0, n_wo)
    def _(num):
        for sub in range(0, SLOT_COLS, COLS):
            cols = pl.ds(pl.multiple_of(num * SLOT_COLS + sub, COLS), COLS)
            out = fdot(attn_ref[...], wo_ref[:, cols])
            h_buf[:, cols] = (h_buf[:, cols].astype(F32) + out).astype(BF16)

    @pl.loop(0, count // 32)
    def _(idx):
        norm_rows(h_buf, b_buf, gain_ref, pl.multiple_of(idx * 32, 32), 32)

    @pl.loop(0, n_ff)
    def _(step):
        num = ff_from + step * group
        half = step // (2 * k_steps)
        kind = lax.rem(step // k_steps, 2)
        k_idx = lax.rem(step, k_steps)
        parts = [take(num + sub, SLOT_ROWS, ff_half) for sub in range(group)]
        lhs = b_buf[:, cols_of(k_idx, SLOT_ROWS * group)]
        for col in range(0, ff_half, COLS):
            size = min(COLS, ff_half - col)
            cols = slice(col, col + size)
            out = fdot(lhs, jnp.concatenate([part[:, cols] for part in parts], axis=0))
            acc_ref[kind, :, cols] = jnp.where(k_idx == 0, 0.0, acc_ref[kind, :, cols]) + out
        for sub in range(group):
            issue(num + sub + SLOTS)

        @pl.when((kind == 1) & (k_idx == k_steps - 1))
        def _():
            for col in range(0, ff_half, 256):
                gate = acc_ref[0, :, col:col + 256]
                dst = pl.ds(pl.multiple_of(half * ff_half + col, 256), 256)
                m_buf[:, dst] = (gate * jax.nn.sigmoid(gate) * acc_ref[1, :, col:col + 256]).astype(BF16)

    def z_copy(blk):
        slot = lax.rem(blk, 2)
        return pltpu.make_async_copy(z_buf.at[slot], z_hbm.at[:, cols_of(blk, dn_cols)], z_sem.at[slot])

    @pl.loop(0, n_dn)
    def _(blk):
        num = dn_from + blk * len(dn_slots)
        parts = []
        for idx, pair in enumerate(dn_slots):
            slot = lax.rem(num + idx, SLOTS)
            for side, rows in enumerate(pair):
                part = slots.at[slot, pl.ds(0, rows), pl.ds(side * dn_cols, dn_cols)]
                pltpu.make_async_copy(part, part, slot_sem.at[slot]).wait()
                parts.append(part)

        @pl.when(blk >= 2)
        def _():
            z_copy(blk - 2).wait()

        for sub in range(0, dn_cols, COLS):
            cols = pl.ds(pl.multiple_of(blk * dn_cols + sub, COLS), COLS)
            out = fdot(m_buf[...], jnp.concatenate([part[:, sub:sub + COLS] for part in parts], axis=0))
            z_buf[lax.rem(blk, 2), :, sub:sub + COLS] = (h_buf[:, cols].astype(F32) + out).astype(BF16)
        z_copy(blk).start()
        for idx in range(len(dn_slots)):
            issue(num + idx + SLOTS)

    for blk in range(max(0, n_dn - 2), n_dn):
        z_copy(blk).wait()


def in_hbm(array):
    return pltpu.with_memory_space_constraint(array, pltpu.HBM)


def in_vmem(array):
    return pltpu.with_memory_space_constraint(array, pltpu.VMEM)


def solution(mesh):
    cp_size = mesh.shape['cp']
    side = math.isqrt(cp_size // 2)
    vmem = pl.BlockSpec(memory_space=pltpu.VMEM)
    hbm = pl.BlockSpec(memory_space=pl.ANY)
    dma = pltpu.SemaphoreType.DMA
    limit = 60 * 1024 * 1024

    def device_fn(x_loc, seg_loc, pos_loc, attn_gain, w_q, w_k, w_v, w_o, mlp_gain, w_gate, w_up, w_down):
        rows = x_loc[0]
        count, depth = rows.shape
        piece = count // 2
        width = w_q.shape[1] // HEAD_DIM * piece
        ff = w_gate.shape[1]
        pos3 = pos_loc.reshape(2, 1, piece)
        freqs = jnp.asarray(rope_freqs()).reshape(HEAD_DIM // 2, 1)
        chunks = depth // SLOT_ROWS
        blocks = count // 32
        table = jax.ShapeDtypeStruct((count, HEAD_DIM), F32)
        cache = jax.ShapeDtypeStruct((count, HEAD_DIM), BF16)
        a_rows, cos_t, sin_t, kv, pos_v, k_rows, v_rows = pl.pallas_call(
            project_kernel,
            out_shape=(jax.ShapeDtypeStruct((count, depth), BF16), table, table, jax.ShapeDtypeStruct((4, piece, HEAD_DIM), BF16), jax.ShapeDtypeStruct((2, 1, piece), jnp.int32), cache, cache),
            in_specs=[hbm, vmem, vmem, vmem, hbm, hbm],
            out_specs=(vmem,) * 7,
            scratch_shapes=[pltpu.VMEM((count, depth), BF16), pltpu.VMEM((depth, HEAD_DIM), BF16), pltpu.VMEM((depth, HEAD_DIM), BF16), dma((blocks,)), dma((2,))],
            compiler_params=pltpu.CompilerParams(vmem_limit_bytes=24 * 1024 * 1024),
            name='project',
        )(in_hbm(rows), in_hbm(attn_gain), in_hbm(pos3), in_hbm(freqs), in_hbm(w_k), in_hbm(w_v))
        attn_rows, wo_near = pl.pallas_call(
            functools.partial(attend_kernel, cp_size, side),
            out_shape=(jax.ShapeDtypeStruct((count, w_q.shape[1]), BF16), jax.ShapeDtypeStruct(w_o.shape, BF16)),
            in_specs=[vmem, vmem, vmem, vmem, vmem, hbm, hbm],
            out_specs=(vmem, vmem),
            scratch_shapes=[pltpu.VMEM((chunks, SLOT_ROWS, w_q.shape[1]), BF16), pltpu.VMEM((2, HEAD_DIM, width), BF16), pltpu.VMEM((cp_size, 4, piece, HEAD_DIM), BF16), pltpu.VMEM((2, 1, width), F32), pltpu.VMEM((2, 1, width), F32), pltpu.VMEM((2, HEAD_DIM, width), F32), pltpu.VMEM((OWNERS * piece, width), F32), dma((chunks,)), dma(()), dma((NUM_COPIES,)), dma((NUM_COPIES,))],
            compiler_params=pltpu.CompilerParams(vmem_limit_bytes=28 * 1024 * 1024, collective_id=0, has_side_effects=True),
            name='attend',
        )(in_vmem(kv), in_vmem(pos_v), in_vmem(cos_t), in_vmem(sin_t), in_vmem(a_rows), in_hbm(w_q), in_hbm(w_o))
        z_rows = pl.pallas_call(
            finish_kernel,
            out_shape=jax.ShapeDtypeStruct((count, depth), BF16),
            in_specs=[hbm, vmem, vmem, vmem, hbm, hbm, hbm],
            out_specs=hbm,
            scratch_shapes=[pltpu.VMEM((count, depth), BF16), pltpu.VMEM((count, depth), BF16), pltpu.VMEM((count, ff), BF16), pltpu.VMEM((2, count, ff // 2), F32), pltpu.VMEM((2, count, SLOT_COLS // 2), BF16), pltpu.VMEM((SLOTS, SLOT_ROWS, SLOT_COLS), BF16), dma(()), dma((SLOTS,)), dma((2,))],
            compiler_params=pltpu.CompilerParams(vmem_limit_bytes=42 * 1024 * 1024),
            name='finish',
        )(in_hbm(rows), in_vmem(attn_rows), in_hbm(mlp_gain), in_vmem(wo_near), w_gate, w_up, w_down)
        return z_rows[None], k_rows[:, None, :], v_rows[:, None, :]

    seq_spec = P(('dp', 'cp'))
    return jax.shard_map(device_fn, mesh=mesh, in_specs=(P('dp', 'cp', None), seq_spec, seq_spec, P(), P(), P(), P(), P(), P(), P(), P(), P()), out_specs=(P('dp', 'cp', None), P(('dp', 'cp'), None, None), P(('dp', 'cp'), None, None)), check_vma=False)
```

```python
import functools
import math

import jax
import jax.numpy as jnp
import numpy as np
from jax import lax
from jax.experimental import pallas as pl
from jax.experimental.pallas import tpu as pltpu
from jax.sharding import PartitionSpec as P

HEAD_DIM = 128
ROPE_THETA = 500000.0
ROPE_FACTOR = 8.0
LOW_FREQ = 1.0
HIGH_FREQ = 4.0
ORIG_CTX = 8192.0
NORM_EPS = 1e-5
NEG_BIG = -1e30
SCORE_LOG2 = HEAD_DIM ** -0.5 * math.log2(math.e)
MESH = pl.DeviceIdType.MESH
COLS = 512
SLOTS = 6
SLOT_ROWS = 1024
SLOT_COLS = 2048
OWNERS = 4
LANES = 256
F32 = jnp.float32
BF16 = jnp.bfloat16


def rope_freqs():
    exponent = np.arange(0, HEAD_DIM, 2) / HEAD_DIM
    inv_freq = 1.0 / (ROPE_THETA ** exponent)
    wavelen = 2.0 * np.pi / inv_freq
    smooth = np.clip((ORIG_CTX / wavelen - LOW_FREQ) / (HIGH_FREQ - LOW_FREQ), 0.0, 1.0)
    return ((1.0 - smooth) * inv_freq / ROPE_FACTOR + smooth * inv_freq).astype(np.float32)


def fdot(lhs, rhs):
    return jnp.dot(lhs, rhs, preferred_element_type=F32)


def norm_rows(src_ref, dst_ref, gain_ref, row, count):
    depth = src_ref.shape[1]
    rows = pl.ds(row, count)
    total = jnp.zeros((count, 128), F32)
    for col in range(0, depth, 128):
        part = src_ref[rows, col:col + 128].astype(F32)
        total = total + part * part
    inv_rms = lax.rsqrt(jnp.sum(total, axis=1, keepdims=True) / depth + NORM_EPS)
    for col in range(0, depth, 512):
        part = src_ref[rows, col:col + 512].astype(F32)
        gain = gain_ref[col:col + 512].astype(F32).reshape(1, 512)
        dst_ref[rows, col:col + 512] = (part * inv_rms * gain).astype(BF16)


def project_kernel(x_hbm, gain_ref, pos_ref, freq_ref, wk_hbm, wv_hbm, a_buf, cos_ref, sin_ref, kv_ref, pos_out, kc_ref, vc_ref, x_buf, wk_buf, wv_buf, x_sem, wkv_sem):
    count = x_buf.shape[0]
    piece = count // 2
    blocks = x_sem.shape[0]
    rows_blk = count // blocks

    def x_copy(idx):
        rows = pl.ds(idx * rows_blk, rows_blk)
        return pltpu.make_async_copy(x_hbm.at[rows], x_buf.at[rows], x_sem.at[idx])

    for idx in range(blocks):
        x_copy(idx).start()
    wkv = [pltpu.make_async_copy(wk_hbm, wk_buf, wkv_sem.at[0]), pltpu.make_async_copy(wv_hbm, wv_buf, wkv_sem.at[1])]
    for copy in wkv:
        copy.start(priority=1)
    pos_out[...] = pos_ref[...]
    for half in range(2):
        rows = slice(half * piece, (half + 1) * piece)
        angles = freq_ref[...] * pos_ref[half].astype(F32)
        cos_h = jnp.cos(angles).T
        sin_h = jnp.sin(angles).T
        cos_ref[rows] = jnp.concatenate([cos_h, cos_h], axis=1)
        sin_ref[rows] = jnp.concatenate([-sin_h, sin_h], axis=1)

    @pl.loop(0, blocks)
    def _(idx):
        x_copy(idx).wait()
        norm_rows(x_buf, a_buf, gain_ref, pl.multiple_of(idx * rows_blk, rows_blk), rows_blk)

    for copy in wkv:
        copy.wait()
    kv_raw = fdot(a_buf[...], jnp.concatenate([wk_buf[...], wv_buf[...]], axis=1))
    k_rot = rope(kv_raw[:, :HEAD_DIM], cos_ref[...], sin_ref[...])
    v_raw = kv_raw[:, HEAD_DIM:]
    kc_ref[...] = k_rot.astype(BF16)
    vc_ref[...] = v_raw.astype(BF16)
    for half in range(2):
        rows = slice(half * piece, (half + 1) * piece)
        kv_ref[half] = k_rot[rows].astype(BF16)
        kv_ref[2 + half] = v_raw[rows].T.astype(BF16)


def rope(raw, cos_t, sin_t):
    half = HEAD_DIM // 2
    return raw * cos_t + jnp.concatenate([raw[:, half:], raw[:, :half]], axis=1) * sin_t


def torus_place(side):
    me = lax.axis_index('cp')
    core = lax.rem(me, 2)
    chip = me // 2
    chip_x = lax.rem(chip, side)
    chip_y = chip // side

    def owner(first, second, core=core):
        pos_x = lax.rem(chip_x + first * (1 - core) + second * core + 2 * side, side)
        pos_y = lax.rem(chip_y + first * core + second * (1 - core) + 2 * side, side)
        return (pos_y * side + pos_x) * 2 + core

    def other(first, second):
        return owner(first, second, 1 - core)

    return me, owner, other


def gather_shards(place, kv_ref, all_ref, send_sem, recv_sem, on_start, on_group):
    me, owner, other = place
    sibling = other(0, 0)
    targets = {'a+': owner(1, 0), 'a-': owner(-1, 0), 'b+': owner(0, 1), 'b-': owner(0, -1), 's': sibling}
    barrier = pltpu.get_barrier_semaphore()
    for target in targets.values():
        pl.semaphore_signal(barrier, inc=1, device_id={'cp': target}, device_id_type=MESH)
    pl.semaphore_wait(barrier, len(targets))

    copies = []

    def send(shard, where, half=None):
        num = len(copies)
        dst = all_ref.at[shard]
        src = kv_ref if num < 5 else dst
        if half is not None:
            dst = dst.at[pl.ds(2 * half, 2)]
            src = dst
        copy = pltpu.make_async_remote_copy(src_ref=src, dst_ref=dst, send_sem=send_sem.at[num], recv_sem=recv_sem.at[num], device_id={'cp': targets[where]}, device_id_type=MESH)
        copy.start()
        copies.append(copy)
        return copy

    from_sibling = []

    def spread(shard):
        plus = send(shard, 'b+')
        minus = send(shard, 'b-')
        from_sibling.append(send(shard, 's'))
        return plus, minus

    def relay(first, row):
        row[0].wait_recv()
        shard = owner(first, -1)
        half_k = send(shard, 'b+', 0)
        from_sibling.append(send(shard, 's'))
        row[1].wait_recv()
        shard = owner(first, 1)
        half_v = send(shard, 'b-', 1)
        from_sibling.append(send(shard, 's'))
        return half_k, half_v

    def close(first, halves):
        halves[0].wait_recv()
        halves[1].wait_recv()
        from_sibling.append(send(owner(first, 2), 's'))

    def arrived(*nums):
        for num in nums:
            from_sibling[num].wait_recv()

    own_right = send(me, 'a+')
    own_left = send(me, 'a-')
    row_own = spread(me)
    all_ref[me] = kv_ref[...]
    own_right.wait_recv()
    shard = owner(-1, 0)
    far_k = send(shard, 'a+', 0)
    row_left = spread(shard)
    own_left.wait_recv()
    shard = owner(1, 0)
    far_v = send(shard, 'a-', 1)
    row_right = spread(shard)
    far_own = relay(0, row_own)
    on_start(0)
    far_k.wait_recv()
    far_v.wait_recv()
    row_far = spread(owner(2, 0))
    on_start(1)
    far_left = relay(-1, row_left)
    far_right = relay(1, row_right)
    arrived(0)
    on_group(me, sibling, owner(-1, 0), owner(1, 0))
    close(0, far_own)
    far_far = relay(2, row_far)
    arrived(1, 2)
    on_group(owner(0, -1), owner(0, 1), other(-1, 0), other(1, 0))
    close(-1, far_left)
    close(1, far_right)
    arrived(3, 4)
    on_group(owner(2, 0), owner(-1, -1), other(0, -1), other(0, 1))
    close(2, far_far)
    arrived(5)
    on_group(owner(-1, 1), owner(1, -1), owner(1, 1), other(2, 0))
    arrived(6, 7)
    on_group(owner(0, 2), owner(2, -1), other(-1, -1), other(-1, 1))
    arrived(8, 9)
    on_group(owner(2, 1), owner(-1, 2), other(1, -1), other(1, 1))
    arrived(10, 11)
    on_group(owner(1, 2), owner(2, 2), other(0, 2), other(2, -1))
    arrived(12, 13, 14, 15)
    on_group(other(2, 1), other(-1, 2), other(1, 2), other(2, 2))
    for copy in copies:
        copy.wait_send()


NUM_COPIES = 36


def attend_kernel(cp_size, side, kv_ref, pos_ref, cos_ref, sin_ref, a_buf, wq_hbm, wo_hbm, out_ref, wo_ref, wq_buf, qt_ref, all_ref, max_ref, sum_ref, acc_ref, score_ref, wq_sem, wo_sem, send_sem, recv_sem):
    place = torus_place(side)
    me = place[0]
    count = a_buf.shape[0]
    piece = count // 2
    width = qt_ref.shape[2]
    tiles = width // LANES
    chunks, chunk_rows = wq_buf.shape[:2]
    loads = [pltpu.make_async_copy(wq_hbm.at[pl.ds(idx * chunk_rows, chunk_rows)], wq_buf.at[idx], wq_sem.at[idx]) for idx in range(chunks)]
    wo_copy = pltpu.make_async_copy(wo_hbm, wo_ref, wo_sem)
    for copy in loads:
        copy.start()

    bases = (me * piece, (2 * cp_size - 1 - me) * piece)
    lane_tok = lax.broadcasted_iota(jnp.int32, (1, piece), 1)

    def starts(half):
        first = bases[half] + lane_tok - pos_ref[half]
        return jnp.concatenate([first] * (LANES // piece), axis=1)

    first_key = (starts(0), starts(1))
    tok = jnp.concatenate([lane_tok] * (LANES // piece), axis=1)
    key_row = lax.broadcasted_iota(jnp.int32, (piece, LANES), 0)

    n_blocks = wq_buf.shape[2] // COLS

    def queries(part):
        if part == 0:
            for copy in loads:
                copy.wait()
            wo_copy.start()
        for col in range(part * n_blocks // 2, (part + 1) * n_blocks // 2):
            q_raw = fdot(a_buf[...], jnp.concatenate([wq_buf[idx, :, col * COLS:(col + 1) * COLS] for idx in range(chunks)], axis=0))
            for sub in range(COLS // HEAD_DIM):
                head = col * (COLS // HEAD_DIM) + sub
                q_rot = rope(q_raw[:, sub * HEAD_DIM:(sub + 1) * HEAD_DIM], cos_ref[...], sin_ref[...])
                for half in range(2):
                    qt_ref[half, :, head * piece:(head + 1) * piece] = q_rot[half * piece:(half + 1) * piece].T.astype(BF16)
        if part == 1:
            for half in range(2):
                visible = (key_row <= tok) & (key_row + bases[half] >= first_key[half])
                for tile in range(tiles):
                    cols = slice(tile * LANES, (tile + 1) * LANES)
                    scores = fdot(kv_ref[half], qt_ref[half, :, cols])
                    scores = jnp.where(visible, scores, NEG_BIG)
                    top = jnp.max(scores, axis=0, keepdims=True)
                    prob = jnp.exp2((scores - top) * SCORE_LOG2)
                    max_ref[half, :, cols] = top
                    sum_ref[half, :, cols] = jnp.sum(prob, axis=0, keepdims=True)
                    acc_ref[half, :, cols] = fdot(kv_ref[2 + half], prob.astype(BF16))

    def block(half, part, owners, key_base):
        keys = jnp.concatenate([all_ref[own, part] for own in owners], axis=0)
        vals = jnp.concatenate([all_ref[own, 2 + part] for own in owners], axis=1)
        hidden = [key_row < first_key[half] - base for base in key_base]
        tops, scales = [], []
        for tile in range(tiles):
            cols = slice(tile * LANES, (tile + 1) * LANES)
            raw = fdot(keys, qt_ref[half, :, cols])
            peak = None
            for sub in range(OWNERS):
                rows = slice(sub * piece, (sub + 1) * piece)
                score = jnp.where(hidden[sub], NEG_BIG, raw[rows])
                score_ref[rows, cols] = score
                best = jnp.max(score, axis=0, keepdims=True)
                peak = best if peak is None else jnp.maximum(peak, best)
            old_top = max_ref[half, :, cols]
            top = jnp.maximum(old_top, peak)
            max_ref[half, :, cols] = top
            tops.append(top)
            scales.append(jnp.exp2((old_top - top) * SCORE_LOG2))
        for tile in range(tiles):
            cols = slice(tile * LANES, (tile + 1) * LANES)
            prob = jnp.exp2((score_ref[:, cols] - tops[tile]) * SCORE_LOG2)
            sum_ref[half, :, cols] = sum_ref[half, :, cols] * scales[tile] + jnp.sum(prob, axis=0, keepdims=True)
            acc_ref[half, :, cols] = acc_ref[half, :, cols] * scales[tile] + fdot(vals, prob.astype(BF16))

    def low_group(*owners):
        block(1, 0, owners, [own * piece for own in owners])

    gather_shards(place, kv_ref, all_ref, send_sem, recv_sem, queries, low_group)

    @pl.loop(0, (me + OWNERS - 1) // OWNERS)
    def _(idx):
        owners = [idx * OWNERS + sub for sub in range(OWNERS)]
        block(0, 0, owners, [jnp.where(own < me, own * piece, -2 * piece) for own in owners])

    @pl.loop((me + 1) // OWNERS, cp_size // OWNERS)
    def _(idx):
        owners = [idx * OWNERS + sub for sub in range(OWNERS)]
        block(1, 1, owners, [jnp.where(own > me, (2 * cp_size - 1 - own) * piece, -2 * piece) for own in owners])

    for half in range(2):
        for head in range(width // piece):
            cols = slice(head * piece, (head + 1) * piece)
            done = acc_ref[half, :, cols] / sum_ref[half, :, cols]
            out_ref[half * piece:(half + 1) * piece, head * HEAD_DIM:(head + 1) * HEAD_DIM] = done.T.astype(BF16)
    wo_copy.wait()


def finish_kernel(x_hbm, attn_ref, gain_ref, wo_ref, wg_hbm, wu_hbm, wd_hbm, z_hbm, h_buf, b_buf, m_buf, acc_ref, z_buf, slots, x_sem, slot_sem, z_sem):
    count, depth = h_buf.shape
    ff = wg_hbm.shape[1]
    ff_half = ff // 2
    group = 2
    n_wo = depth // SLOT_COLS
    k_steps = depth // (SLOT_ROWS * group)
    n_ff = 4 * k_steps
    dn_cols = SLOT_COLS // 2
    dn_rows = [min(SLOT_ROWS, ff - row) for row in range(0, ff, SLOT_ROWS)]
    dn_slots = [dn_rows[idx:idx + 2] for idx in range(0, len(dn_rows), 2)]
    n_dn = depth // dn_cols
    ff_from = 0
    dn_from = ff_from + n_ff * group
    total = dn_from + n_dn * len(dn_slots)

    def cols_of(idx, size):
        return pl.ds(pl.multiple_of(idx * size, size), size)

    def halves(src, dst, rows, sem):
        for part in range(2):
            sel = pl.ds(part * rows // 2, rows // 2)
            pltpu.make_async_copy(src.at[sel], dst.at[sel], sem).start(priority=part)

    def issue(num):
        slot = lax.rem(num, SLOTS)
        sem = slot_sem.at[slot]
        dst = slots.at[slot]

        rel = num - ff_from
        step = rel // group
        half = step // (2 * k_steps)
        kind = lax.rem(step // k_steps, 2)
        row = cols_of(lax.rem(step, k_steps) * group + lax.rem(rel, group), SLOT_ROWS)
        in_ff = (num >= ff_from) & (num < dn_from)

        @pl.when(in_ff & (kind == 0))
        def _():
            halves(wg_hbm.at[row, cols_of(half, ff_half)], dst.at[:, pl.ds(0, ff_half)], SLOT_ROWS, sem)

        @pl.when(in_ff & (kind == 1))
        def _():
            halves(wu_hbm.at[row, cols_of(half, ff_half)], dst.at[:, pl.ds(0, ff_half)], SLOT_ROWS, sem)

        rel = num - dn_from
        for idx, pair in enumerate(dn_slots):
            @pl.when((num >= dn_from) & (num < total) & (lax.rem(rel, len(dn_slots)) == idx))
            def _():
                for side, rows in enumerate(pair):
                    src = wd_hbm.at[pl.ds((2 * idx + side) * SLOT_ROWS, rows), cols_of(rel // len(dn_slots), dn_cols)]
                    pltpu.make_async_copy(src, dst.at[pl.ds(0, rows), pl.ds(side * dn_cols, dn_cols)], sem).start(priority=side)

    def take(num, rows, cols):
        slot = lax.rem(num, SLOTS)
        part = slots.at[slot, pl.ds(0, rows), pl.ds(0, cols)]
        pltpu.make_async_copy(part, part, slot_sem.at[slot]).wait()
        return slots.at[slot]

    x_copy = pltpu.make_async_copy(x_hbm, h_buf, x_sem)
    x_copy.start()
    for num in range(SLOTS):
        issue(jnp.int32(num))
    x_copy.wait()

    @pl.loop(0, n_wo)
    def _(num):
        for sub in range(0, SLOT_COLS, COLS):
            cols = pl.ds(pl.multiple_of(num * SLOT_COLS + sub, COLS), COLS)
            out = fdot(attn_ref[...], wo_ref[:, cols])
            h_buf[:, cols] = (h_buf[:, cols].astype(F32) + out).astype(BF16)

    @pl.loop(0, count // 32)
    def _(idx):
        norm_rows(h_buf, b_buf, gain_ref, pl.multiple_of(idx * 32, 32), 32)

    @pl.loop(0, n_ff)
    def _(step):
        num = ff_from + step * group
        half = step // (2 * k_steps)
        kind = lax.rem(step // k_steps, 2)
        k_idx = lax.rem(step, k_steps)
        parts = [take(num + sub, SLOT_ROWS, ff_half) for sub in range(group)]
        lhs = b_buf[:, cols_of(k_idx, SLOT_ROWS * group)]
        for col in range(0, ff_half, COLS):
            size = min(COLS, ff_half - col)
            cols = slice(col, col + size)
            out = fdot(lhs, jnp.concatenate([part[:, cols] for part in parts], axis=0))
            acc_ref[kind, :, cols] = jnp.where(k_idx == 0, 0.0, acc_ref[kind, :, cols]) + out
        for sub in range(group):
            issue(num + sub + SLOTS)

        @pl.when((kind == 1) & (k_idx == k_steps - 1))
        def _():
            for col in range(0, ff_half, 256):
                gate = acc_ref[0, :, col:col + 256]
                dst = pl.ds(pl.multiple_of(half * ff_half + col, 256), 256)
                m_buf[:, dst] = (gate * jax.nn.sigmoid(gate) * acc_ref[1, :, col:col + 256]).astype(BF16)

    def z_copy(blk):
        slot = lax.rem(blk, 2)
        return pltpu.make_async_copy(z_buf.at[slot], z_hbm.at[:, cols_of(blk, dn_cols)], z_sem.at[slot])

    @pl.loop(0, n_dn)
    def _(blk):
        num = dn_from + blk * len(dn_slots)
        parts = []
        for idx, pair in enumerate(dn_slots):
            slot = lax.rem(num + idx, SLOTS)
            for side, rows in enumerate(pair):
                part = slots.at[slot, pl.ds(0, rows), pl.ds(side * dn_cols, dn_cols)]
                pltpu.make_async_copy(part, part, slot_sem.at[slot]).wait()
                parts.append(part)

        @pl.when(blk >= 2)
        def _():
            z_copy(blk - 2).wait()

        for sub in range(0, dn_cols, COLS):
            cols = pl.ds(pl.multiple_of(blk * dn_cols + sub, COLS), COLS)
            out = fdot(m_buf[...], jnp.concatenate([part[:, sub:sub + COLS] for part in parts], axis=0))
            z_buf[lax.rem(blk, 2), :, sub:sub + COLS] = (h_buf[:, cols].astype(F32) + out).astype(BF16)
        z_copy(blk).start()
        for idx in range(len(dn_slots)):
            issue(num + idx + SLOTS)

    for blk in range(max(0, n_dn - 2), n_dn):
        z_copy(blk).wait()


def in_hbm(array):
    return pltpu.with_memory_space_constraint(array, pltpu.HBM)


def in_vmem(array):
    return pltpu.with_memory_space_constraint(array, pltpu.VMEM)


def solution(mesh):
    cp_size = mesh.shape['cp']
    side = math.isqrt(cp_size // 2)
    vmem = pl.BlockSpec(memory_space=pltpu.VMEM)
    hbm = pl.BlockSpec(memory_space=pl.ANY)
    dma = pltpu.SemaphoreType.DMA
    limit = 60 * 1024 * 1024

    def device_fn(x_loc, seg_loc, pos_loc, attn_gain, w_q, w_k, w_v, w_o, mlp_gain, w_gate, w_up, w_down):
        rows = x_loc[0]
        count, depth = rows.shape
        piece = count // 2
        width = w_q.shape[1] // HEAD_DIM * piece
        ff = w_gate.shape[1]
        pos3 = pos_loc.reshape(2, 1, piece)
        freqs = jnp.asarray(rope_freqs()).reshape(HEAD_DIM // 2, 1)
        chunks = depth // SLOT_ROWS
        blocks = count // 32
        table = jax.ShapeDtypeStruct((count, HEAD_DIM), F32)
        cache = jax.ShapeDtypeStruct((count, HEAD_DIM), BF16)
        a_rows, cos_t, sin_t, kv, pos_v, k_rows, v_rows = pl.pallas_call(
            project_kernel,
            out_shape=(jax.ShapeDtypeStruct((count, depth), BF16), table, table, jax.ShapeDtypeStruct((4, piece, HEAD_DIM), BF16), jax.ShapeDtypeStruct((2, 1, piece), jnp.int32), cache, cache),
            in_specs=[hbm, vmem, vmem, vmem, hbm, hbm],
            out_specs=(vmem,) * 7,
            scratch_shapes=[pltpu.VMEM((count, depth), BF16), pltpu.VMEM((depth, HEAD_DIM), BF16), pltpu.VMEM((depth, HEAD_DIM), BF16), dma((blocks,)), dma((2,))],
            compiler_params=pltpu.CompilerParams(vmem_limit_bytes=24 * 1024 * 1024),
            name='project',
        )(in_hbm(rows), in_hbm(attn_gain), in_hbm(pos3), in_hbm(freqs), in_hbm(w_k), in_hbm(w_v))
        attn_rows, wo_near = pl.pallas_call(
            functools.partial(attend_kernel, cp_size, side),
            out_shape=(jax.ShapeDtypeStruct((count, w_q.shape[1]), BF16), jax.ShapeDtypeStruct(w_o.shape, BF16)),
            in_specs=[vmem, vmem, vmem, vmem, vmem, hbm, hbm],
            out_specs=(vmem, vmem),
            scratch_shapes=[pltpu.VMEM((chunks, SLOT_ROWS, w_q.shape[1]), BF16), pltpu.VMEM((2, HEAD_DIM, width), BF16), pltpu.VMEM((cp_size, 4, piece, HEAD_DIM), BF16), pltpu.VMEM((2, 1, width), F32), pltpu.VMEM((2, 1, width), F32), pltpu.VMEM((2, HEAD_DIM, width), F32), pltpu.VMEM((OWNERS * piece, width), F32), dma((chunks,)), dma(()), dma((NUM_COPIES,)), dma((NUM_COPIES,))],
            compiler_params=pltpu.CompilerParams(vmem_limit_bytes=28 * 1024 * 1024, collective_id=0, has_side_effects=True),
            name='attend',
        )(in_vmem(kv), in_vmem(pos_v), in_vmem(cos_t), in_vmem(sin_t), in_vmem(a_rows), in_hbm(w_q), in_hbm(w_o))
        z_rows = pl.pallas_call(
            finish_kernel,
            out_shape=jax.ShapeDtypeStruct((count, depth), BF16),
            in_specs=[hbm, vmem, vmem, vmem, hbm, hbm, hbm],
            out_specs=hbm,
            scratch_shapes=[pltpu.VMEM((count, depth), BF16), pltpu.VMEM((count, depth), BF16), pltpu.VMEM((count, ff), BF16), pltpu.VMEM((2, count, ff // 2), F32), pltpu.VMEM((2, count, SLOT_COLS // 2), BF16), pltpu.VMEM((SLOTS, SLOT_ROWS, SLOT_COLS), BF16), dma(()), dma((SLOTS,)), dma((2,))],
            compiler_params=pltpu.CompilerParams(vmem_limit_bytes=42 * 1024 * 1024),
            name='finish',
        )(in_hbm(rows), in_vmem(attn_rows), in_hbm(mlp_gain), in_vmem(wo_near), w_gate, w_up, w_down)
        return z_rows[None], k_rows[:, None, :], v_rows[:, None, :]

    seq_spec = P(('dp', 'cp'))
    return jax.shard_map(device_fn, mesh=mesh, in_specs=(P('dp', 'cp', None), seq_spec, seq_spec, P(), P(), P(), P(), P(), P(), P(), P(), P()), out_specs=(P('dp', 'cp', None), P(('dp', 'cp'), None, None), P(('dp', 'cp'), None, None)), check_vma=False)
```
